32 devices in a mesh: seq: 4 (over y, x), fsdp: 8 (over z, core).
Axes of the slice: x: 2, y: 2, z: 4, core: 2. Of those that a mesh axis runs over, the one named last changes fastest.
Arguments:
- tokens: bfloat16 [8, 512, 8192], P('fsdp', 'seq'), may hold values from -6 to 6
- norm_gain: float32 [8192], replicated, may hold values from 0.3 to 3
- w_query: bfloat16 [8192, 4096], P(('seq', 'fsdp')), may hold values from -1 to 1
- key_weight: bfloat16 [8192, 512], P(('seq', 'fsdp')), may hold values from -1 to 1
- value_weight: bfloat16 [8192, 512], P(('seq', 'fsdp')), may hold values from -0.0625 to 0.0625
- w_out: bfloat16 [4096, 8192], P(None, ('seq', 'fsdp')), may hold values from -0.09375 to 0.09375
Outputs:
- result: float32 [8, 512, 8192], P('fsdp', 'seq')
The draws below stay inside these ranges and needn't reach their ends.
All inputs are finite; a program needn't handle non-finite values.
Results may differ from the reference program's by a relative error of at most 0.04.
Values may be sent and summed in bfloat16 or wider, within the bound.
A program may use at most 128 MiB of HBM per device.

```python
import math
import jax
import jax.numpy as jnp
from jax import lax

MODEL_WIDTH = 8192
HQ = 32
KEY_VALUE_HEADS = 4
HEAD_SIZE = 128
GROUP = 8
SEQUENCE_TOKENS = 512
SEQS = 8
N_SEQ = 4


def projection_sample(key, head_count):
    normal_draw = jax.random.normal(jax.random.fold_in(key, 11), (MODEL_WIDTH, head_count * HEAD_SIZE), jnp.float32)
    normal_draw = jnp.clip(normal_draw, -6.0, 6.0) / math.sqrt(MODEL_WIDTH)
    normal_draw = jnp.clip(normal_draw, -1.0, 1.0)
    return normal_draw.astype(jnp.bfloat16)


def draw_w_query(key, part):
    return projection_sample(jax.random.fold_in(key, 101), HQ)


def draw_key_weight(key, part):
    return projection_sample(jax.random.fold_in(key, 202), KEY_VALUE_HEADS)


def shard_levels(rng, extent, split, smallest, top_value):
    def one(position, parts):
        heights = jax.random.uniform(jax.random.fold_in(jax.random.fold_in(rng, 6), position), (parts,), jnp.float32, smallest / len(split), top_value / len(split))
        return jnp.repeat(jnp.exp(heights), extent[position] // parts).reshape((-1,) + (1,) * (len(extent) - position - 1))

    level = one(*split[0])
    for cut in split[1:]:
        level = level * one(*cut)
    return level


def bell_draw(own_key, extent, deviation, bound, shards=(), kind=jnp.bfloat16):
    entries = jax.random.normal(own_key, extent, jnp.float32) * deviation
    if len(shards) > 0:
        entries = shard_levels(own_key, extent, shards, -0.22, 0.18) * entries
    return jnp.clip(entries, min=-bound, max=bound).astype(kind)


def setup_inputs(seed: int = 0) -> dict:
    splits = jax.random.split(jax.random.key(seed), 7)
    tokens = bell_draw(splits[0], (SEQS, SEQUENCE_TOKENS, MODEL_WIDTH), 1.0, 6.0, ((0, 8), (1, 4)))
    norm_gain = jnp.clip(jnp.exp(jax.random.uniform(splits[1], (MODEL_WIDTH,), jnp.float32, math.log(0.3), math.log(3.0))), 0.3, 3.0)
    w_query = draw_w_query(jax.random.fold_in(splits[6], 71), 0)
    key_weight = draw_key_weight(jax.random.fold_in(splits[6], 71), 0)
    value_weight = bell_draw(splits[4], (MODEL_WIDTH, KEY_VALUE_HEADS * HEAD_SIZE), MODEL_WIDTH ** -0.5, 0.0625, ((0, 32),))
    w_out = bell_draw(splits[5], (HQ * HEAD_SIZE, MODEL_WIDTH), (HQ * HEAD_SIZE) ** -0.5, 0.09375, ((1, 32),))
    return {"tokens": tokens, "norm_gain": norm_gain, "w_query": w_query, "key_weight": key_weight, "value_weight": value_weight, "w_out": w_out}


def rms_norm(sequence_rows, norm_gain):
    floats = sequence_rows.astype(jnp.float32)
    mean_square = lax.optimization_barrier(jnp.mean(floats * floats, axis=-1, keepdims=True))
    return (floats * lax.rsqrt(mean_square + 1e-05) * norm_gain).astype(jnp.bfloat16)

def apply_projection(normed_input, weight):
    block = MODEL_WIDTH // N_SEQ
    running = jnp.zeros((normed_input.shape[0], weight.shape[1]), jnp.float32)
    for block_index in range(N_SEQ):
        partial_sum = jnp.dot(normed_input[:, block_index * block:(block_index + 1) * block], weight[block_index * block:(block_index + 1) * block], preferred_element_type=jnp.float32)
        rounded = lax.optimization_barrier(partial_sum.astype(jnp.bfloat16))
        running = running + rounded.astype(jnp.float32)
    return running.astype(jnp.bfloat16)

def reference(tokens, norm_gain, w_query, key_weight, value_weight, w_out):
    scale = HEAD_SIZE ** (-0.5)
    row_ids = lax.broadcasted_iota(jnp.int32, (SEQUENCE_TOKENS, SEQUENCE_TOKENS), 0)
    col_ids = lax.broadcasted_iota(jnp.int32, (SEQUENCE_TOKENS, SEQUENCE_TOKENS), 1)
    causal = row_ids >= col_ids

    def one_sequence(sequence_rows):
        normed_input = rms_norm(sequence_rows, norm_gain)
        queries = apply_projection(normed_input, w_query).reshape(SEQUENCE_TOKENS, HQ, HEAD_SIZE)
        key_tensor = apply_projection(normed_input, key_weight).reshape(SEQUENCE_TOKENS, KEY_VALUE_HEADS, HEAD_SIZE)
        value_tensor = apply_projection(normed_input, value_weight).reshape(SEQUENCE_TOKENS, KEY_VALUE_HEADS, HEAD_SIZE)

        def one_head(head_index):
            query_head = lax.dynamic_index_in_dim(queries, head_index, 1, keepdims=False)
            kv_index = head_index // GROUP
            key_head = lax.dynamic_index_in_dim(key_tensor, kv_index, 1, keepdims=False)
            value_head = lax.dynamic_index_in_dim(value_tensor, kv_index, 1, keepdims=False)
            scores = jnp.dot(query_head, key_head.T, preferred_element_type=jnp.float32) * scale
            scores = jnp.where(causal, scores, jnp.float32(-1e+30))
            top = lax.optimization_barrier(jnp.max(scores, axis=-1, keepdims=True))
            weights = jnp.exp(scores - top)
            probs = (weights / lax.optimization_barrier(jnp.sum(weights, axis=-1, keepdims=True))).astype(jnp.bfloat16)
            return jnp.dot(probs, value_head, preferred_element_type=jnp.float32).astype(jnp.bfloat16)
        heads = lax.map(one_head, jnp.arange(HQ, dtype=jnp.int32))
        heads = jnp.transpose(heads, (1, 0, 2)).reshape(SEQUENCE_TOKENS, HQ * HEAD_SIZE)
        branch = jnp.dot(heads, w_out, preferred_element_type=jnp.float32).astype(jnp.bfloat16)
        return sequence_rows.astype(jnp.float32) + branch.astype(jnp.float32)
    return lax.map(one_sequence, tokens)
```

```python
import functools

import jax
import jax.numpy as jnp
from jax import lax
from jax.experimental import pallas as pl
from jax.experimental.pallas import tpu as pltpu
from jax.sharding import PartitionSpec as P

HEAD = 128
CORES = 2
PAIR = 2
SLOTS = 3
PIECES = 8
FILL = 1
MESH = pl.DeviceIdType.MESH
F32, BF16 = jnp.float32, jnp.bfloat16


class Plan:
    def __init__(self, group, devices, tokens, w_query, key_weight, w_out):
        self.group, self.devices = group, devices
        self.stops = devices // CORES
        self.fold = self.stops == 4
        self.turns = 2 if self.fold else 1
        self.count, self.features = tokens.shape
        self.width = self.features // group
        self.depth = self.width // devices
        self.length = self.count * group
        self.rows_out, self.cols_out = w_out.shape
        heads = w_query.shape[1] // HEAD
        self.group_heads = heads // (key_weight.shape[1] // HEAD)
        self.local_heads = heads // group
        self.local_width = self.local_heads * HEAD
        self.chunk = PAIR * HEAD
        self.chunks = 1 + self.local_heads // PAIR
        self.flat = self.cols_out % HEAD == 0


def when(condition, action):
    if condition is True:
        action()
    else:
        pl.when(condition)(action)


def flip(index, mask):
    result, bit = index, 1
    while bit < 8:
        side = 1 - 2 * ((index // bit) % 2)
        result = result + ((mask // bit) % 2) * bit * side
        bit *= 2
    return result


def orders(turn, group):
    bits = []
    while 2 ** len(bits) < group:
        bits.append(2 ** len(bits))
    return bits[turn:] + bits[:turn]


def kernel(plan, tokens, gain, wq, wk, wv, wo, out, gathered,
           tok, gw, nrm, part, recv, fin, ret, heads, nv, br,
           w_rx, w_in, w_out, w_sib, w_loc, n_rx, n_in, n_out, n_sib,
           x_rx, x_tx, x_loc, g_rx, g_tx, r_rx, r_tx, ret_rx, ret_tx,
           h_rx, h_tx, b_rx, b_tx, b_loc, nv_sem):
    G, S, C = plan.group, plan.stops, plan.chunks
    cw, depth, width, count = plan.chunk, plan.depth, plan.width, plan.count
    length, lw, fold, turns = plan.length, plan.local_width, plan.fold, plan.turns
    seq = lax.axis_index("seq")
    fsdp = lax.axis_index("fsdp")
    stop, core = fsdp // CORES, fsdp % CORES
    half = stop // (S // 2)
    toward = 1 - 2 * half
    far = half * (S - 1) + toward * stop
    inward = (seq, (stop + toward) * CORES + core)
    outward = (seq, (stop - toward) * CORES + core)
    sibling = (seq, stop * CORES + 1 - core)
    host = far >= 1 if fold else True
    pending = []

    def remote(source, target, send, receive, device):
        return pltpu.make_async_remote_copy(
            src_ref=source, dst_ref=target, send_sem=send, recv_sem=receive,
            device_id=device, device_id_type=MESH)

    def send(condition, make):
        when(condition, lambda: make().start())
        pending.append((condition, make))

    def origin(i):
        return jnp.where(far >= i, stop - i * toward, stop + (i - far) * toward)

    def rows(start, size):
        return pl.ds(pl.multiple_of(start * size, size), size)

    def block(j, o, c):
        return gw.at[j, rows(o * CORES + c, depth), :]

    def w_inward(j, o):
        b = block(j, o, core)
        return remote(b, b, w_in.at[j, o], w_rx.at[j, o, core], inward)

    def w_outward(j, o):
        b = block(j, o, core)
        return remote(b, b, w_out.at[j, o], w_rx.at[j, o, core], outward)

    def w_across(j, o):
        b = block(j, o, core)
        return remote(b, b, w_sib.at[j, o], w_rx.at[j, o, core], sibling)

    def w_arrive(i, j):
        o = origin(i)

        def take():
            b = block(j, o, core)
            remote(b, b, w_sib.at[j, o], w_rx.at[j, o, core], sibling).wait_recv()

        when(host, take)
        if i <= S // 2 - 1:
            send(far >= i, lambda: w_inward(j, o))
        if not fold:
            send((far < i) & (far >= 1), lambda: w_outward(j, o))
        send(host, lambda: w_across(j, o))

    def w_own_in(condition, j):
        send(condition, lambda: w_inward(j, stop))

    def w_other_core(j):
        def take():
            for i in range(S):
                o = stop if i == 0 else origin(i)
                b = block(j, o, 1 - core)
                remote(b, b, w_sib.at[j, o], w_rx.at[j, o, 1 - core], sibling).wait_recv()

        when(host, take)

    piece = plan.rows_out // PIECES

    def n_source(o, pc, own):
        cut = pl.ds(pc * piece, piece)
        return wo.at[cut, :] if own else gathered.at[o * CORES + core, cut, :]

    def n_target(o, c, pc):
        return gathered.at[o * CORES + c, pl.ds(pc * piece, piece), :]

    def n_copy(o, pc, own, sems, device):
        return remote(n_source(o, pc, own), n_target(o, core, pc),
                      sems.at[o, pc], n_rx.at[o, core, pc], device)

    def n_own_in(condition, pc):
        send(condition, lambda: n_copy(stop, pc, True, n_in, inward))

    def n_wait(o, c, pc):
        t = n_target(o, c, pc)
        remote(t, t, n_sib.at[o, pc], n_rx.at[o, c, pc], sibling).wait_recv()

    def n_arrive(i, pc):
        o = origin(i)
        n_wait(o, core, pc)
        if i <= S // 2 - 1:
            send(far >= i, lambda: n_copy(o, pc, False, n_in, inward))
        send((far < i) & (far >= 1), lambda: n_copy(o, pc, False, n_out, outward))
        send(True, lambda: n_copy(o, pc, False, n_sib, sibling))

    barrier = pltpu.get_barrier_semaphore()

    def greet(device):
        pl.semaphore_signal(barrier, inc=1, device_id=device, device_id_type=MESH)

    for k in range(1, G):
        greet((flip(seq, k), fsdp))
    greet(sibling)
    greet(inward)
    pl.when(far >= 1)(lambda: greet(outward))

    mine = rows(fsdp, depth)
    for j in range(C):
        for d in range(G):
            if j == 0:
                kv = pl.ds(d * plan.local_heads // plan.group_heads * HEAD, HEAD)
                for side, w in enumerate((wk, wv)):
                    spot = pl.ds(d * cw + side * HEAD, HEAD)
                    pltpu.make_async_copy(w.at[:, kv], gw.at[0, mine, spot], w_loc.at[0]).start()
            else:
                part_of = pl.ds(d * lw + (j - 1) * cw, cw)
                pltpu.make_async_copy(
                    wq.at[:, part_of], gw.at[j, mine, pl.ds(d * cw, cw)], w_loc.at[j]).start()
    load = pltpu.make_async_copy(tokens, tok, x_loc.at[0])
    load.start()

    pl.semaphore_wait(barrier, G + 1 + (far + S // 2 - 1) // (S // 2))

    for j in range(C):
        own = gw.at[j, mine, :]
        pltpu.make_async_copy(own, own, w_loc.at[j]).wait()
        if j == 0:
            w_own_in(True, 0)
        elif j == 1:
            w_own_in(host, 1)
        if not fold:
            send(far >= 1, lambda j=j: w_outward(j, stop))
        send(host, lambda j=j: w_across(j, stop))
    for pc in range(PIECES):
        send(far >= 1, lambda pc=pc: n_copy(stop, pc, True, n_out, outward))

    load.wait()

    def norm_rows(i, carry):
        r = rows(i, 16)
        x = tok[r, :].astype(F32)
        mean = jnp.mean(x * x, axis=-1, keepdims=True)
        tok[r, :] = (x * lax.rsqrt(mean + 1e-05) * gain[...]).astype(BF16)
        return carry

    lax.fori_loop(0, count // 16, norm_rows, 0)

    def x_copy(k):
        d = flip(seq, k)
        return remote(tok.at[:, rows(d, width)], nrm.at[0, rows(seq, count), :],
                      x_tx.at[k], x_rx.at[k], (d, fsdp))

    own_x = pltpu.make_async_copy(
        tok.at[:, rows(seq, width)], nrm.at[0, rows(seq, count), :], x_loc.at[1])
    own_x.start()
    for k in range(1, G):
        send(True, lambda k=k: x_copy(k))

    def x_wait(k):
        if k == 0:
            own_x.wait()
        else:
            spot = nrm.at[0, rows(flip(seq, k), count), :]
            remote(spot, spot, x_tx.at[k], x_rx.at[k], sibling).wait_recv()

    def g_copy(k):
        r = rows(flip(seq, k), count)
        return remote(nrm.at[0, r, :], nrm.at[turns - 1, r, :], g_tx.at[k], g_rx.at[k], inward)

    guest = far < 1
    if fold:
        for k in range(G):
            pl.when(guest)(lambda k=k: x_wait(k))
            send(guest, lambda k=k: g_copy(k))
        for j in range(1, C):
            w_own_in(guest, j)
        for pc in range(PIECES):
            n_own_in(guest, pc)

    def project(j, low, high):
        def step(i, carry):
            t, u = i // G, i % G
            bit = t + 1
            first = 1 - u // (G // 2)
            v = (G - 1 - u) % (G // 2)
            k = (v // bit) * (2 * bit) + first * bit + v % bit
            slot = j % SLOTS
            acc = jnp.dot(nrm[t], gw[j, :, rows(flip(seq, k), cw)], preferred_element_type=F32)
            part[slot, t, k] = acc.astype(BF16)

            @pl.when(first == 1)
            def _():
                remote(part.at[slot, t, k], recv.at[j, t, v], r_tx.at[j, t, k],
                       r_rx.at[j, t, v], (flip(seq, bit), fsdp)).start()

            return carry

        lax.fori_loop(low * G, high * G, step, 0)

    def alive(t, q):
        bits = orders(t, G)[:q]
        return [k for k in range(G) if not any(k & b for b in bits)]

    def landing(t, q, k):
        return sum(len(alive(t, p + 1)) for p in range(q)) + alive(t, q + 1).index(k)

    stages = len(orders(0, G))

    def r_wait(j, t, q, k):
        n = landing(t, q, k)
        spot = recv.at[j, t, n]
        remote(spot, spot, r_tx.at[j, t, 1], r_rx.at[j, t, n], sibling).wait_recv()

    def total(j, t, upto, k, store):
        tile = 64

        def step(i, carry):
            r = rows(i, tile)
            value = part[j % SLOTS, t, k, r, :].astype(F32)
            for q in range(upto):
                value = value + recv[j, t, landing(t, q, k), r, :].astype(F32)
            store(r, value.astype(BF16))
            return carry

        lax.fori_loop(0, length // tile, step, 0)

    def stage(j, q):
        for t in range(turns):
            bit = orders(t, G)[q]
            for k in alive(t, q):
                r_wait(j, t, q - 1, k)
            for k in reversed(alive(t, q)):
                if k & bit:
                    def put(r, value, t=t, k=k):
                        part[j % SLOTS, t, k, r, :] = value

                    total(j, t, q, k, put)
                    n = landing(t, q, k ^ bit)
                    remote(part.at[j % SLOTS, t, k], recv.at[j, t, n], r_tx.at[j, t, k],
                           r_rx.at[j, t, n], (flip(seq, bit), fsdp)).start()

    def ret_copy(j):
        return remote(ret.at[j], fin.at[j], ret_tx.at[j], ret_rx.at[j], outward)

    def settle(j):
        def take():
            for t in reversed(range(turns)):
                r_wait(j, t, stages - 1, 0)

                def put(r, value, t=t):
                    if t:
                        ret[j, r, :] = value
                    else:
                        fin[j, r, :] = value

                total(j, t, stages, 0, put)
                if t:
                    ret_copy(j).start()

        when(host, take)
        if fold:
            pending.append((host, lambda: ret_copy(j)))
            pl.when(guest)(lambda: remote(fin.at[j], fin.at[j], ret_tx.at[j], ret_rx.at[j],
                                          sibling).wait_recv())

    def h_copy(j, k):
        spot = heads.at[:, rows(seq * (C - 1) + j - 1, cw)]
        return remote(spot, spot, h_tx.at[j, k], h_rx.at[j, k], (flip(seq, k), fsdp))

    def attend(j):
        tile = 256

        def one_head(h, carry):
            column = rows(h, HEAD)
            for i in range(length // tile):
                seen = (i + 1) * tile
                q = fin[j, pl.ds(i * tile, tile), column]
                scores = lax.dot_general(
                    q, fin[0, pl.ds(0, seen), pl.ds(0, HEAD)],
                    (((1,), (1,)), ((), ())), preferred_element_type=F32) * (HEAD ** -0.5)
                row = lax.broadcasted_iota(jnp.int32, (tile, seen), 0) + i * tile
                col = lax.broadcasted_iota(jnp.int32, (tile, seen), 1)
                scores = jnp.where(row >= col, scores, F32(-1e30))
                top = jnp.max(scores, axis=-1, keepdims=True)
                weights = jnp.exp(scores - top)
                probs = weights * (1.0 / jnp.sum(weights, axis=-1, keepdims=True))
                mixed = jnp.dot(probs.astype(BF16), fin[0, pl.ds(0, seen), pl.ds(HEAD, HEAD)],
                                preferred_element_type=F32)
                spot = rows((seq * (C - 1) + j - 1) * PAIR + h, HEAD)
                heads[pl.ds(i * tile, tile), spot] = mixed.astype(BF16)
            return carry

        lax.fori_loop(0, PAIR, one_head, 0)
        for k in range(1, G):
            send(True, lambda k=k: h_copy(j, k))

    def target(c):
        b = seq * plan.devices + c
        return out.at[:, rows(b, plan.cols_out)] if plan.flat else out.at[b]

    def branch(o, own):
        for n in range(CORES):
            b = o * CORES + (core if n == 0 else 1 - core)
            source = wo if own and n == 0 else gathered.at[b]
            pltpu.make_async_copy(source, nv.at[n], nv_sem.at[n]).start()
        tile = 256
        for n in range(CORES):
            b = o * CORES + (core if n == 0 else 1 - core)
            pltpu.make_async_copy(wo, nv.at[n], nv_sem.at[n]).wait()

            def step(i, carry):
                r = rows(i, tile)
                acc = jnp.dot(heads[r, :], nv[n], preferred_element_type=F32)
                br[b, r, :] = acc.astype(BF16)
                return carry

            lax.fori_loop(0, length // tile, step, 0)
            for k in range(1, G):
                d = flip(seq, k)
                remote(br.at[b, rows(d, count), :], target(b), b_tx.at[k], b_rx.at[k],
                       (d, fsdp)).start()
            pltpu.make_async_copy(br.at[b, rows(seq, count), :], target(b), b_loc.at[0]).start()

    def host_first():
        for k in range(G):
            x_wait(k)
        project(0, 0, 1)
        if fold:
            for k in range(G):
                r = nrm.at[1, rows(flip(seq, k), count), :]
                remote(r, r, g_tx.at[k], g_rx.at[k], sibling).wait_recv()
            project(0, 1, 2)

    ahead = 0

    def prefetch(last):
        nonlocal ahead
        while ahead <= min(last, C - 1):
            w_arrive(1, ahead)
            ahead += 1

    prefetch(0)
    for j in range(2, C):
        w_own_in(host, j)
    for pc in range(FILL):
        n_own_in(host, pc)
    for i in range(2, S):
        w_arrive(i, 0)
    for pc in range(PIECES):
        send(True, lambda pc=pc: n_copy(stop, pc, True, n_sib, sibling))
    w_other_core(0)
    when(host, host_first)
    prefetch(1)
    filled = False
    for j in range(1, C):
        for i in range(2, S - 1):
            w_arrive(i, j)
        prefetch(j + 1)
        if S > 2:
            w_arrive(S - 1, j)
        prefetch(j + 2)
        if ahead == C and not filled:
            filled = True
            for pc in range(FILL, PIECES):
                n_own_in(host, pc)
        w_other_core(j)

        def middle(j=j):
            if j >= SLOTS:
                for t in range(turns):
                    for k in range(1, G):
                        p = part.at[j % SLOTS, t, k]
                        remote(p, p, r_tx.at[j - SLOTS, t, k], r_rx.at[j, t, 0], sibling).wait_send()
            project(j, 0, turns)
            for q in range(1, stages):
                stage(j - 1, q)

        when(host, middle)
        if j >= 2:
            settle(j - 2)
            if j >= 3:
                attend(j - 2)

    arrivals = [(i, pc) for i in range(1, S) for pc in range(PIECES)]
    taken = []

    def polls(wanted):
        for i, pc in wanted:
            if (i, pc) not in taken and i < S:
                taken.append((i, pc))
                n_arrive(i, pc)

    quarter = PIECES // 4
    polls([(1, pc) for pc in range(2 * quarter)])

    def last_stages():
        for q in range(1, stages):
            stage(C - 1, q)

    when(host, last_stages)
    polls([(2, pc) for pc in range(2 * quarter)])
    if C >= 2:
        settle(C - 2)
        if C >= 3:
            attend(C - 2)
    polls([(1, pc) for pc in range(PIECES)])
    polls([(2, pc) for pc in range(3 * quarter)])
    settle(C - 1)
    attend(C - 1)
    polls([(2, pc) for pc in range(PIECES)])
    polls([(3, pc) for pc in range(quarter)])
    for j in range(1, C):
        for k in range(1, G):
            spot = heads.at[:, rows(flip(seq, k) * (C - 1) + j - 1, cw)]
            remote(spot, spot, h_tx.at[j, k], h_rx.at[j, k], sibling).wait_recv()
    for pc in range(PIECES):
        n_wait(stop, 1 - core, pc)
    branch(stop, True)
    for i in range(1, S):
        polls([(i, pc) for pc in range(PIECES)])
        for pc in range(PIECES):
            n_wait(origin(i), 1 - core, pc)
        branch(origin(i), False)

    def all_of(side):
        span = plan.devices * plan.cols_out
        return out.at[:, rows(side, span)] if plan.flat else out.at[rows(side, plan.devices)]

    for k in range(1, G):
        remote(all_of(seq), all_of(flip(seq, k)), b_tx.at[k], b_rx.at[k], sibling).wait()
    pltpu.make_async_copy(all_of(seq), all_of(seq), b_loc.at[0]).wait()
    for condition, make in pending:
        when(condition, lambda make=make: make().wait_send())

    def drain():
        for j in range(max(0, C - SLOTS), C):
            for t in range(turns):
                for k in range(1, G):
                    p = part.at[j % SLOTS, t, k]
                    remote(p, p, r_tx.at[j, t, k], r_rx.at[j, t, 0], sibling).wait_send()

    when(host, drain)


def body(tokens, norm_gain, w_query, key_weight, value_weight, w_out):
    group, devices = lax.axis_size("seq"), lax.axis_size("fsdp")
    plan = Plan(group, devices, tokens[0], w_query, key_weight, w_out)
    G, S, C, T = plan.group, plan.stops, plan.chunks, plan.turns
    length, cw = plan.length, plan.chunk
    any_space = pl.BlockSpec(memory_space=pl.ANY)
    dma = pltpu.SemaphoreType.DMA
    if plan.flat:
        out_shape = (plan.count, plan.features)
    else:
        out_shape = (G * devices, plan.count, plan.cols_out)
    outward = (1, 1) if plan.fold else (C, S)
    branches, _ = pl.pallas_call(
        functools.partial(kernel, plan),
        out_shape=(
            jax.ShapeDtypeStruct(out_shape, BF16),
            jax.ShapeDtypeStruct((devices,) + w_out.shape, BF16),
        ),
        in_specs=[any_space, pl.BlockSpec(memory_space=pltpu.VMEM)] + [any_space] * 4,
        out_specs=(any_space, any_space),
        scratch_shapes=[
            pltpu.VMEM((plan.count, plan.features), BF16),
            pltpu.VMEM((C, plan.width, G * cw), BF16),
            pltpu.VMEM((T, length, plan.width), BF16),
            pltpu.VMEM((SLOTS, T, G, length, cw), BF16),
            pltpu.VMEM((C, T, G - 1, length, cw), BF16),
            pltpu.VMEM((C, length, cw), BF16),
            pltpu.VMEM((C if plan.fold else 1, length, cw), BF16),
            pltpu.VMEM((length, plan.rows_out), BF16),
            pltpu.VMEM((CORES,) + w_out.shape, BF16),
            pltpu.VMEM((devices, length, plan.cols_out), BF16),
            dma((C, S, CORES)), dma((C, S)), dma(outward), dma((C, S)), dma((C,)),
            dma((S, CORES, PIECES)), dma((S, PIECES)), dma((S, PIECES)), dma((S, PIECES)),
            dma((G,)), dma((G,)), dma((2,)), dma((G,)), dma((G,)),
            dma((C, T, G)), dma((C, T, G)), dma((C,)), dma((C,)),
            dma((C, G)), dma((C, G)), dma((G,)), dma((G,)), dma((1,)), dma((CORES,)),
        ],
        compiler_params=pltpu.CompilerParams(
            collective_id=0, has_side_effects=True, vmem_limit_bytes=67043328),
    )(tokens[0], norm_gain[None], w_query, key_weight, value_weight, w_out)
    if not plan.flat:
        branches = jnp.transpose(branches, (1, 0, 2)).reshape(plan.count, plan.features)
    return tokens.astype(F32) + branches[None].astype(F32)


def solution(mesh):
    placed = (
        P("fsdp", "seq", None),
        P(),
        P(("seq", "fsdp"), None),
        P(("seq", "fsdp"), None),
        P(("seq", "fsdp"), None),
        P(None, ("seq", "fsdp")),
    )
    return jax.shard_map(
        body, mesh=mesh, in_specs=placed, out_specs=P("fsdp", "seq", None), check_vma=False
    )
```

```python
import functools

import jax
import jax.numpy as jnp
from jax import lax
from jax.experimental import pallas as pl
from jax.experimental.pallas import tpu as pltpu
from jax.sharding import PartitionSpec as P

HEAD = 128
CORES = 2
PAIR = 2
SLOTS = 3
PIECES = 8
FILL = 6
MESH = pl.DeviceIdType.MESH
F32, BF16 = jnp.float32, jnp.bfloat16


class Plan:
    def __init__(self, group, devices, tokens, w_query, key_weight, w_out):
        self.group, self.devices = group, devices
        self.stops = devices // CORES
        self.fold = self.stops == 4
        self.turns = 2 if self.fold else 1
        self.count, self.features = tokens.shape
        self.width = self.features // group
        self.depth = self.width // devices
        self.length = self.count * group
        self.rows_out, self.cols_out = w_out.shape
        heads = w_query.shape[1] // HEAD
        self.group_heads = heads // (key_weight.shape[1] // HEAD)
        self.local_heads = heads // group
        self.local_width = self.local_heads * HEAD
        self.chunk = PAIR * HEAD
        self.chunks = 1 + self.local_heads // PAIR
        self.flat = self.cols_out % HEAD == 0
        self.parts = self.cols_out // HEAD if self.flat else 1
        self.part_cols = self.cols_out // self.parts
        self.part_rows = PIECES // self.parts
        self.units = 1 if self.flat else CORES


def when(condition, action):
    def run():
        action()

    if condition is True:
        run()
    else:
        pl.when(condition)(run)


def both_true(one, other):
    return other if one is True else one & other


def flip(index, mask):
    result, bit = index, 1
    while bit < 8:
        side = 1 - 2 * ((index // bit) % 2)
        result = result + ((mask // bit) % 2) * bit * side
        bit *= 2
    return result


def orders(turn, group):
    bits = []
    while 2 ** len(bits) < group:
        bits.append(2 ** len(bits))
    return bits[turn:] + bits[:turn]


def kernel(plan, tokens, gain, wq, wk, wv, wo, out, gathered,
           tok, gw, nrm, part, recv, fin, ret, heads, nv, br, br_acc,
           w_rx, w_in, w_out, w_sib, w_loc, n_rx, n_in, n_out, n_sib,
           x_rx, x_tx, x_loc, g_rx, g_tx, r_rx, r_tx, ret_rx, ret_tx,
           h_rx, h_tx, b_rx, b_tx, b_loc, nv_sem):
    G, S, C = plan.group, plan.stops, plan.chunks
    cw, depth, width, count = plan.chunk, plan.depth, plan.width, plan.count
    length, lw, fold, turns = plan.length, plan.local_width, plan.fold, plan.turns
    seq = lax.axis_index("seq")
    fsdp = lax.axis_index("fsdp")
    stop, core = fsdp // CORES, fsdp % CORES
    half = stop // (S // 2)
    toward = 1 - 2 * half
    far = half * (S - 1) + toward * stop
    inward = (seq, (stop + toward) * CORES + core)
    outward = (seq, (stop - toward) * CORES + core)
    sibling = (seq, stop * CORES + 1 - core)
    host = far >= 1 if fold else True
    pending = []

    def remote(source, target, send, receive, device):
        return pltpu.make_async_remote_copy(
            src_ref=source, dst_ref=target, send_sem=send, recv_sem=receive,
            device_id=device, device_id_type=MESH)

    def send(condition, make):
        when(condition, lambda: make().start())
        pending.append((condition, make))

    def origin(i):
        return jnp.where(far >= i, stop - i * toward, stop + (i - far) * toward)

    def rows(start, size):
        return pl.ds(pl.multiple_of(start * size, size), size)

    def block(j, o, c):
        return gw.at[j, rows(o * CORES + c, depth), :]

    def w_inward(j, o):
        b = block(j, o, core)
        return remote(b, b, w_in.at[j, o], w_rx.at[j, o, core], inward)

    def w_outward(j, o):
        b = block(j, o, core)
        return remote(b, b, w_out.at[j, o], w_rx.at[j, o, core], outward)

    def w_across(j, o):
        b = block(j, o, core)
        return remote(b, b, w_sib.at[j, o], w_rx.at[j, o, core], sibling)

    def w_arrive(i, j):
        with jax.named_scope(f"w{i}_{j}"):
            w_arrive_body(i, j)

    def w_arrive_body(i, j):
        o = origin(i)

        def take():
            b = block(j, o, core)
            remote(b, b, w_sib.at[j, o], w_rx.at[j, o, core], sibling).wait_recv()

        when(host, take)
        if i <= S // 2 - 1:
            send(far >= i, lambda: w_inward(j, o))
        if not fold:
            send((far < i) & (far >= 1), lambda: w_outward(j, o))
        send(host, lambda: w_across(j, o))

    def w_own_in(condition, j):
        send(condition, lambda: w_inward(j, stop))

    def w_other_core(j):
        with jax.named_scope(f"wsib_{j}"):
            w_other_core_body(j)

    def w_other_core_body(j):
        def take():
            for i in range(S):
                o = stop if i == 0 else origin(i)
                b = block(j, o, 1 - core)
                remote(b, b, w_sib.at[j, o], w_rx.at[j, o, 1 - core], sibling).wait_recv()

        when(host, take)

    per_part = plan.part_rows
    piece = plan.rows_out // per_part
    pw = plan.part_cols

    def n_cut(pc):
        return pl.ds(pc % per_part * piece, piece), pl.ds(pc // per_part * pw, pw)

    def n_source(o, pc, own):
        r, c = n_cut(pc)
        return wo.at[r, c] if own else gathered.at[o * CORES + core, r, c]

    def n_target(o, c, pc):
        r, cut = n_cut(pc)
        return gathered.at[o * CORES + c, r, cut]

    def n_copy(o, pc, own, sems, device):
        return remote(n_source(o, pc, own), n_target(o, core, pc),
                      sems.at[o, pc], n_rx.at[o, core, pc], device)

    def n_own_in(condition, pc):
        send(condition, lambda: n_copy(stop, pc, True, n_in, inward))

    def n_wait(o, c, pc):
        t = n_target(o, c, pc)
        remote(t, t, n_sib.at[o, pc], n_rx.at[o, c, pc], sibling).wait_recv()

    def n_arrive(i, pc, who=True):
        o = origin(i)

        def take():
            with jax.named_scope(f"n{i}_{pc}"):
                n_wait(o, core, pc)

        when(who, take)
        if i <= S // 2 - 1:
            send(both_true(who, far >= i), lambda: n_copy(o, pc, False, n_in, inward))
        send(both_true(who, (far < i) & (far >= 1)),
             lambda: n_copy(o, pc, False, n_out, outward))
        send(who, lambda: n_copy(o, pc, False, n_sib, sibling))

    barrier = pltpu.get_barrier_semaphore()

    def greet(device):
        pl.semaphore_signal(barrier, inc=1, device_id=device, device_id_type=MESH)

    for k in range(1, G):
        greet((flip(seq, k), fsdp))
    greet(sibling)
    greet(inward)
    pl.when(far >= 1)(lambda: greet(outward))

    mine = rows(fsdp, depth)
    for j in range(C):
        for d in range(G):
            if j == 0:
                kv = pl.ds(d * plan.local_heads // plan.group_heads * HEAD, HEAD)
                for side, w in enumerate((wk, wv)):
                    spot = pl.ds(d * cw + side * HEAD, HEAD)
                    pltpu.make_async_copy(w.at[:, kv], gw.at[0, mine, spot], w_loc.at[0]).start()
            else:
                part_of = pl.ds(d * lw + (j - 1) * cw, cw)
                pltpu.make_async_copy(
                    wq.at[:, part_of], gw.at[j, mine, pl.ds(d * cw, cw)], w_loc.at[j]).start()
    load = pltpu.make_async_copy(tokens, tok, x_loc.at[0])
    load.start()

    pl.semaphore_wait(barrier, G + 1 + (far + S // 2 - 1) // (S // 2))

    for j in range(C):
        own = gw.at[j, mine, :]
        pltpu.make_async_copy(own, own, w_loc.at[j]).wait()
        if j == 0:
            w_own_in(True, 0)
        elif j == 1:
            w_own_in(True, 1)
        if not fold:
            send(far >= 1, lambda j=j: w_outward(j, stop))
        send(host, lambda j=j: w_across(j, stop))
    for pc in range(PIECES):
        send(far >= 1, lambda pc=pc: n_copy(stop, pc, True, n_out, outward))

    load.wait()

    def norm_rows(i, carry):
        r = rows(i, 16)
        x = tok[r, :].astype(F32)
        mean = jnp.mean(x * x, axis=-1, keepdims=True)
        tok[r, :] = (x * lax.rsqrt(mean + 1e-05) * gain[...]).astype(BF16)
        return carry

    lax.fori_loop(0, count // 16, norm_rows, 0)

    def x_copy(k):
        d = flip(seq, k)
        return remote(tok.at[:, rows(d, width)], nrm.at[0, rows(seq, count), :],
                      x_tx.at[k], x_rx.at[k], (d, fsdp))

    own_x = pltpu.make_async_copy(
        tok.at[:, rows(seq, width)], nrm.at[0, rows(seq, count), :], x_loc.at[1])
    own_x.start()
    for k in range(1, G):
        send(True, lambda k=k: x_copy(k))

    def x_wait(k):
        if k == 0:
            own_x.wait()
        else:
            spot = nrm.at[0, rows(flip(seq, k), count), :]
            remote(spot, spot, x_tx.at[k], x_rx.at[k], sibling).wait_recv()

    def g_copy(k):
        r = rows(flip(seq, k), count)
        return remote(nrm.at[0, r, :], nrm.at[turns - 1, r, :], g_tx.at[k], g_rx.at[k], inward)

    guest = far < 1
    if fold:
        for k in range(G):
            pl.when(guest)(lambda k=k: x_wait(k))
            send(guest, lambda k=k: g_copy(k))
        for j in range(2, C):
            w_own_in(guest, j)
        for pc in range(PIECES):
            n_own_in(guest, pc)

    def project(j, low, high):
        with jax.named_scope(f"project_{j}"):
            project_body(j, low, high)

    def project_body(j, low, high):
        def step(i, carry):
            t, k = i // G, G - 1 - i % G
            slot = j % SLOTS
            acc = jnp.dot(nrm[t], gw[j, :, rows(flip(seq, k), cw)], preferred_element_type=F32)
            for u in range(PAIR):
                part[slot, t, u, k] = acc[:, u * HEAD:(u + 1) * HEAD].astype(BF16)
            for u in range(PAIR):
                bit = u + 1

                @pl.when((k // bit) % 2 == 1)
                def _(u=u, bit=bit):
                    n = (k // (2 * bit)) * bit + k % bit
                    remote(part.at[slot, t, u, k], recv.at[j, t, u, n], r_tx.at[j, t, u, k],
                           r_rx.at[j, t, u, n], (flip(seq, bit), fsdp)).start()

            return carry

        lax.fori_loop(low * G, high * G, step, 0)

    def alive(u, q):
        bits = orders(u, G)[:q]
        return [k for k in range(G) if not any(k & b for b in bits)]

    def landing(u, q, k):
        return sum(len(alive(u, p + 1)) for p in range(q)) + alive(u, q + 1).index(k)

    stages = len(orders(0, G))

    def r_wait(j, t, u, q, k):
        n = landing(u, q, k)
        spot = recv.at[j, t, u, n]
        remote(spot, spot, r_tx.at[j, t, u, 1], r_rx.at[j, t, u, n], sibling).wait_recv()

    def total(j, t, u, upto, k, store):
        tile = 128
        for q in range(upto):
            r_wait(j, t, u, q, k)

        def step(i, carry):
            r = rows(i, tile)
            value = part[j % SLOTS, t, u, k, r, :].astype(F32)
            for q in range(upto):
                value = value + recv[j, t, u, landing(u, q, k), r, :].astype(F32)
            store(r, value.astype(BF16))
            return carry

        lax.fori_loop(0, length // tile, step, 0)

    def stage(j, t):
        with jax.named_scope(f"stage_{j}_{t}"):
            stage_body(j, t)

    def stage_body(j, t):
        for q in range(1, stages):
            for u in range(PAIR):
                bit = orders(u, G)[q]
                for k in reversed(alive(u, q)):
                    if k & bit:
                        def put(r, value, u=u, k=k):
                            part[j % SLOTS, t, u, k, r, :] = value

                        total(j, t, u, q, k, put)
                        n = landing(u, q, k ^ bit)
                        remote(part.at[j % SLOTS, t, u, k], recv.at[j, t, u, n],
                               r_tx.at[j, t, u, k], r_rx.at[j, t, u, n],
                               (flip(seq, bit), fsdp)).start()

    def ret_copy(j):
        return remote(ret.at[j], fin.at[j], ret_tx.at[j], ret_rx.at[j], outward)

    def settle(j, t):
        with jax.named_scope(f"settle_{j}_{t}"):
            settle_body(j, t)

    def settle_body(j, t):
        for u in range(PAIR):
            def put(r, value, u=u):
                if t:
                    ret[j, r, pl.ds(u * HEAD, HEAD)] = value
                else:
                    fin[j, r, pl.ds(u * HEAD, HEAD)] = value

            total(j, t, u, stages, 0, put)
        if t:
            ret_copy(j).start()

    def returned(j):
        if fold:
            pending.append((host, lambda: ret_copy(j)))

            @pl.when(guest)
            def _():
                with jax.named_scope(f"returned_{j}"):
                    remote(fin.at[j], fin.at[j], ret_tx.at[j], ret_rx.at[j], sibling).wait_recv()

    def sent(j):
        for t in range(turns):
            for u in range(PAIR):
                for k in range(1, G):
                    p = part.at[j % SLOTS, t, u, k]
                    remote(p, p, r_tx.at[j, t, u, k], r_rx.at[j, t, u, 0], sibling).wait_send()

    relayed = G == 4
    near = [1, 2] if relayed else list(range(1, G))

    def h_spot(owner, j):
        return heads.at[:, rows(owner * (C - 1) + j - 1, cw)]

    def h_half(owner, j, u):
        return heads.at[:, rows((owner * (C - 1) + j - 1) * PAIR + u, HEAD)]

    def h_copy(j, k):
        spot = h_spot(seq, j)
        return remote(spot, spot, h_tx.at[j, k], h_rx.at[j, k], (flip(seq, k), fsdp))

    def h_relay(j, u):
        came, goes = orders(u, G)[:2]
        half = h_half(flip(seq, came), j, u)
        return remote(half, half, h_tx.at[j, G + u], h_rx.at[j, G + u], (flip(seq, goes), fsdp))

    def h_wait(j):
        with jax.named_scope(f"hwait_{j}"):
            for k in near:
                spot = h_spot(flip(seq, k), j)
                remote(spot, spot, h_tx.at[j, k], h_rx.at[j, k], sibling).wait_recv()

    def relay(j):
        h_wait(j)
        if relayed:
            for u in range(PAIR):
                send(True, lambda u=u: h_relay(j, u))

    def h_last(j):
        if relayed:
            with jax.named_scope(f"hlast_{j}"):
                for u in range(PAIR):
                    half = h_half(flip(seq, G - 1), j, u)
                    remote(half, half, h_tx.at[j, G + u], h_rx.at[j, G + u], sibling).wait_recv()

    def attend(j, condition=True):
        when(condition, lambda: mix(j))
        for k in near:
            pending.append((condition, lambda k=k: h_copy(j, k)))

    def mix(j):
        with jax.named_scope(f"attend_{j}"):
            mix_body(j)

    def mix_body(j):
        tile = 256

        def one_head(h, carry):
            column = rows(h, HEAD)
            for i in range(length // tile):
                seen = (i + 1) * tile
                q = fin[j, pl.ds(i * tile, tile), column]
                scores = lax.dot_general(
                    q, fin[0, pl.ds(0, seen), pl.ds(0, HEAD)],
                    (((1,), (1,)), ((), ())), preferred_element_type=F32) * (HEAD ** -0.5)
                row = lax.broadcasted_iota(jnp.int32, (tile, seen), 0) + i * tile
                col = lax.broadcasted_iota(jnp.int32, (tile, seen), 1)
                scores = jnp.where(row >= col, scores, F32(-1e30))
                top = jnp.max(scores, axis=-1, keepdims=True)
                weights = jnp.exp(scores - top)
                probs = weights * (1.0 / jnp.sum(weights, axis=-1, keepdims=True))
                mixed = jnp.dot(probs.astype(BF16), fin[0, pl.ds(0, seen), pl.ds(HEAD, HEAD)],
                                preferred_element_type=F32)
                spot = rows((seq * (C - 1) + j - 1) * PAIR + h, HEAD)
                heads[pl.ds(i * tile, tile), spot] = mixed.astype(BF16)
            return carry

        lax.fori_loop(0, PAIR, one_head, 0)
        for k in near:
            h_copy(j, k).start()

    def target(c, h):
        b = seq * plan.devices + c
        if not plan.flat:
            return out.at[b]
        return out.at[:, rows(b * plan.parts + h, pw)]

    def n_spot(h, c, r):
        if plan.flat:
            return nv.at[h, 0, r, pl.ds(c * pw, pw)]
        return nv.at[h, c, r, :]

    def n_load(o, own, h, r):
        copies = []
        for n in range(CORES):
            c = core if n == 0 else 1 - core
            cut = pl.ds(h * pw, pw)
            source = wo.at[r, cut] if own and n == 0 else gathered.at[o * CORES + c, r, cut]
            copies.append(pltpu.make_async_copy(source, n_spot(h, n, r), nv_sem.at[h, n]))
        return copies

    def br_spot(o, h, n, r):
        if plan.flat:
            return br.at[o, h, 0, r, pl.ds(n * pw, pw)]
        return br.at[o, h, n, r, :]

    def br_send(o, h):
        for n in range(CORES):
            c = core if n == 0 else 1 - core
            for k in range(1, G):
                d = flip(seq, k)
                remote(br_spot(o, h, n, rows(d, count)), target(o * CORES + c, h),
                       b_tx.at[k], b_rx.at[k], (d, fsdp)).start()
            pltpu.make_async_copy(br_spot(o, h, n, rows(seq, count)), target(o * CORES + c, h),
                                  b_loc.at[0]).start()

    tile = 256
    whole = pl.ds(0, plan.rows_out)

    def branch(o, own):
        with jax.named_scope("branch"):
            branch_body(o, own)

    def branch_body(o, own):
        copies = [n_load(o, own, h, whole) for h in range(plan.parts)]
        for pair in copies:
            for copy in pair:
                copy.start()
        for h in range(plan.parts):
            for copy in copies[h]:
                copy.wait()
            for unit in range(plan.units):
                def step(i, carry, h=h, unit=unit):
                    r = rows(i, tile)
                    acc = jnp.dot(heads[r, :], nv[h, unit], preferred_element_type=F32)
                    br[o, h, unit, r, :] = acc.astype(BF16)
                    return carry

                lax.fori_loop(0, length // tile, step, 0)
            br_send(o, h)

    def branch_last(i):
        o = origin(i)
        for pc in range(PIECES):
            polls(i, pc, pc + 2)
            with jax.named_scope(f"nsib_{i}_{pc}"):
                n_wait(o, 1 - core, pc)
            h, q = pc // per_part, pc % per_part
            copies = n_load(o, False, h, pl.ds(q * piece, piece))
            for copy in copies:
                copy.start()
            for copy in copies:
                copy.wait()
            for unit in range(plan.units):
                def step(i, carry, h=h, q=q, unit=unit):
                    r = rows(i, tile)
                    cut = pl.ds(q * piece, piece)
                    acc = jnp.dot(heads[r, cut], nv[h, unit, cut, :], preferred_element_type=F32)
                    if q:
                        acc = acc + br_acc[unit, r, :]
                    if q < per_part - 1:
                        br_acc[unit, r, :] = acc
                    else:
                        br[o, h, unit, r, :] = acc.astype(BF16)
                    return carry

                lax.fori_loop(0, length // tile, step, 0)
            if q == per_part - 1:
                br_send(o, h)

    def both(action):
        for t in range(turns):
            action(t)

    early = min(2, C)

    def both_early(action):
        for j in range(early):
            action(j, 1)

    def take_chunk(j):
        for i in range(2, S):
            w_arrive(i, j)
        w_other_core(j)

    for j in range(early):
        w_arrive(1, j)
    for pc in range(FILL):
        n_own_in(host, pc)
    if early < C:
        w_own_in(host, early)
    for j in range(early):
        take_chunk(j)
        if j == 0:
            when(host, lambda: [x_wait(k) for k in range(G)])
        when(host, lambda j=j: project(j, 0, 1))
        if j == 0:
            for pc in range(PIECES):
                send(True, lambda pc=pc: n_copy(stop, pc, True, n_sib, sibling))

    def own_early():
        for j in range(early):
            stage(j, 0)
        for j in range(early):
            settle(j, 0)
        for j in range(1, early):
            mix(j)

    def guests_early():
        with jax.named_scope("gwait"):
            for k in range(G):
                r = nrm.at[1, rows(flip(seq, k), count), :]
                remote(r, r, g_tx.at[k], g_rx.at[k], sibling).wait_recv()
        for j in range(early):
            project(j, 1, 2)

    when(host, own_early)
    for j in range(1, early):
        for k in near:
            pending.append((host, lambda j=j, k=k: h_copy(j, k)))
    taken = []
    relays = [j for j in range(1, C)]

    def polls(i, first, last, role=None):
        for pc in range(first * PIECES // 8, min(last, 8) * PIECES // 8):
            for who, name in ((host, "host"), (guest, "guest")):
                if (i, pc, name) in taken or i >= S or role not in (None, name):
                    continue
                if name == "host" and role is None and (i, pc, "guest") not in taken:
                    taken.extend([(i, pc, "host"), (i, pc, "guest")])
                    n_arrive(i, pc)
                elif name == "host" or fold:
                    taken.append((i, pc, name))
                    n_arrive(i, pc, who)

    def gather(i):
        polls(i, 0, 8)
        with jax.named_scope(f"nsib_{i}"):
            for pc in range(PIECES):
                n_wait(origin(i), 1 - core, pc)

    def relay_to(j):
        while relays and relays[0] <= j:
            relay(relays.pop(0))

    def close(j):
        when(host, lambda: both(lambda t: settle(j, t)))
        returned(j)

    def forward(j):
        if early <= j < C:
            w_arrive(1, j)
            if j + 1 < C:
                w_own_in(host, j + 1)

    polls(2, 0, 2, "host")
    if fold:
        when(host, guests_early)
    polls(2, 2, 5, "host")
    forward(early)
    if fold:
        when(host, lambda: both_early(stage))
    polls(2, 5, FILL, "host")
    if fold:
        when(host, lambda: both_early(settle))
    for j in range(early + 1, C):
        forward(j)
    for pc in range(FILL, PIECES):
        n_own_in(host, pc)
    if fold:
        polls(1, 0, 8, "guest")
        polls(2, 0, FILL, "guest")
        for e in range(early):
            returned(e)
        for e in range(1, early):
            attend(e, guest)
    waiting = None
    for j in range(early, C):
        take_chunk(j)
        if j >= SLOTS:
            when(host, lambda j=j: sent(j - SLOTS))
        when(host, lambda j=j: project(j, 0, turns))
        if j == C - 1:
            polls(1, 6, 8, "host")
            polls(2, 6, 7, "host")
        if waiting is not None:
            close(waiting)
        relay_to(j - 2)
        when(host, lambda j=j: both(lambda t: stage(j, t)))
        if j == C - 1:
            polls(2, 7, 8, "host")
        if waiting is not None:
            attend(waiting)
        waiting = j
        if j < C - 2:
            close(j)
            attend(j)
            waiting = None
        if j == C - 2:
            polls(1, 0, 6, "host")
    polls(3, 0, 1, "host")
    polls(2, 0, 8, "guest")
    if waiting is not None:
        close(waiting)
        attend(waiting)
    polls(3, 1, 2, "host")
    relay_to(C - 2)
    polls(3, 2, 3, "host")
    relay_to(C - 1)
    polls(3, 3, 4, "host")
    polls(3, 0, 2, "guest")
    for j in range(1, C):
        h_last(j)
    for pc in range(PIECES):
        n_wait(stop, 1 - core, pc)
    branch(stop, True)
    polls(3, 4, 5, "host")
    polls(3, 2, 3, "guest")
    for i in range(1, S - 1):
        gather(i)
        branch(origin(i), False)
        polls(3, 4 + i, 5 + i, "host")
        polls(3, 2 + i, 3 + i, "guest")
    polls(3, 0, 8, "host")
    if S > 1:
        branch_last(S - 1)

    def all_of(side):
        span = plan.devices * plan.cols_out
        return out.at[:, rows(side, span)] if plan.flat else out.at[rows(side, plan.devices)]

    with jax.named_scope("sends"):
        for condition, make in pending:
            when(condition, lambda make=make: make().wait_send())
        when(host, lambda: [sent(j) for j in range(max(0, C - SLOTS), C)])
    with jax.named_scope("bwait"):
        for k in range(1, G):
            remote(all_of(seq), all_of(flip(seq, k)), b_tx.at[k], b_rx.at[k], sibling).wait()
        pltpu.make_async_copy(all_of(seq), all_of(seq), b_loc.at[0]).wait()


def body(tokens, norm_gain, w_query, key_weight, value_weight, w_out):
    group, devices = lax.axis_size("seq"), lax.axis_size("fsdp")
    plan = Plan(group, devices, tokens[0], w_query, key_weight, w_out)
    G, S, C, T = plan.group, plan.stops, plan.chunks, plan.turns
    length, cw = plan.length, plan.chunk
    unit_cols = plan.part_cols * CORES // plan.units
    any_space = pl.BlockSpec(memory_space=pl.ANY)
    dma = pltpu.SemaphoreType.DMA
    if plan.flat:
        out_shape = (plan.count, plan.features)
    else:
        out_shape = (G * devices, plan.count, plan.cols_out)
    outward = (1, 1) if plan.fold else (C, S)
    branches, _ = pl.pallas_call(
        functools.partial(kernel, plan),
        out_shape=(
            jax.ShapeDtypeStruct(out_shape, BF16),
            jax.ShapeDtypeStruct((devices,) + w_out.shape, BF16),
        ),
        in_specs=[any_space, pl.BlockSpec(memory_space=pltpu.VMEM)] + [any_space] * 4,
        out_specs=(any_space, any_space),
        scratch_shapes=[
            pltpu.VMEM((plan.count, plan.features), BF16),
            pltpu.VMEM((C, plan.width, G * cw), BF16),
            pltpu.VMEM((T, length, plan.width), BF16),
            pltpu.VMEM((SLOTS, T, PAIR, G, length, HEAD), BF16),
            pltpu.VMEM((C, T, PAIR, G - 1, length, HEAD), BF16),
            pltpu.VMEM((C, length, cw), BF16),
            pltpu.VMEM((C if plan.fold else 1, length, cw), BF16),
            pltpu.VMEM((length, plan.rows_out), BF16),
            pltpu.VMEM((plan.parts, plan.units, plan.rows_out, unit_cols), BF16),
            pltpu.VMEM((S, plan.parts, plan.units, length, unit_cols), BF16),
            pltpu.VMEM((plan.units, length, unit_cols), F32),
            dma((C, S, CORES)), dma((C, S)), dma(outward), dma((C, S)), dma((C,)),
            dma((S, CORES, PIECES)), dma((S, PIECES)), dma((S, PIECES)), dma((S, PIECES)),
            dma((G,)), dma((G,)), dma((2,)), dma((G,)), dma((G,)),
            dma((C, T, PAIR, G)), dma((C, T, PAIR, G)), dma((C,)), dma((C,)),
            dma((C, G + PAIR)), dma((C, G + PAIR)), dma((G,)), dma((G,)), dma((1,)), dma((plan.parts, CORES)),
        ],
        compiler_params=pltpu.CompilerParams(
            collective_id=0, has_side_effects=True, vmem_limit_bytes=67043328),
    )(tokens[0], norm_gain[None], w_query, key_weight, value_weight, w_out)
    if not plan.flat:
        branches = jnp.transpose(branches, (1, 0, 2)).reshape(plan.count, plan.features)
    return tokens.astype(F32) + branches[None].astype(F32)


def solution(mesh):
    placed = (
        P("fsdp", "seq", None),
        P(),
        P(("seq", "fsdp"), None),
        P(("seq", "fsdp"), None),
        P(("seq", "fsdp"), None),
        P(None, ("seq", "fsdp")),
    )
    return jax.shard_map(
        body, mesh=mesh, in_specs=placed, out_specs=P("fsdp", "seq", None), check_vma=False
    )
```

```python
import functools

import jax
import jax.numpy as jnp
from jax import lax
from jax.experimental import pallas as pl
from jax.experimental.pallas import tpu as pltpu
from jax.sharding import PartitionSpec as P

HEAD = 128
CORES = 2
PAIR = 2
SLOTS = 2
PIECES = 8
FILL = 4
MESH = pl.DeviceIdType.MESH
F32, BF16 = jnp.float32, jnp.bfloat16


class Plan:
    def __init__(self, group, devices, tokens, w_query, key_weight, w_out):
        self.group, self.devices = group, devices
        self.stops = devices // CORES
        self.fold = self.stops == 4
        self.turns = 2 if self.fold else 1
        self.count, self.features = tokens.shape
        self.width = self.features // group
        self.depth = self.width // devices
        self.length = self.count * group
        self.rows_out, self.cols_out = w_out.shape
        heads = w_query.shape[1] // HEAD
        self.group_heads = heads // (key_weight.shape[1] // HEAD)
        self.local_heads = heads // group
        self.local_width = self.local_heads * HEAD
        self.chunk = PAIR * HEAD
        self.chunks = 1 + self.local_heads // PAIR
        self.flat = self.cols_out % HEAD == 0
        self.parts = self.cols_out // HEAD if self.flat else 1
        self.part_cols = self.cols_out // self.parts
        self.part_rows = PIECES // self.parts
        self.units = 1 if self.flat else CORES
        self.kept = self.stops - 1 if self.fold else 1


def when(condition, action):
    def run():
        action()

    if condition is True:
        run()
    else:
        pl.when(condition)(run)


def both_true(one, other):
    return other if one is True else one & other


def flip(index, mask):
    result, bit = index, 1
    while bit < 8:
        side = 1 - 2 * ((index // bit) % 2)
        result = result + ((mask // bit) % 2) * bit * side
        bit *= 2
    return result


def orders(turn, group):
    bits = []
    while 2 ** len(bits) < group:
        bits.append(2 ** len(bits))
    return bits[turn:] + bits[:turn]


def kernel(plan, tokens, gain, wq, wk, wv, wo, out, gathered,
           tok, gw, nrm, part, recv, fin, ret, heads, nv, nv_late, br, br_acc,
           w_rx, w_in, w_out, w_sib, w_loc, n_rx, n_in, n_out, n_sib,
           x_rx, x_tx, x_loc, g_rx, g_tx, r_rx, r_tx, ret_rx, ret_tx,
           h_rx, h_tx, b_rx, b_tx, b_loc, nv_sem, nl_sem):
    G, S, C = plan.group, plan.stops, plan.chunks
    cw, depth, width, count = plan.chunk, plan.depth, plan.width, plan.count
    length, lw, fold, turns = plan.length, plan.local_width, plan.fold, plan.turns
    seq = lax.axis_index("seq")
    fsdp = lax.axis_index("fsdp")
    stop, core = fsdp // CORES, fsdp % CORES
    half = stop // (S // 2)
    toward = 1 - 2 * half
    far = half * (S - 1) + toward * stop
    inward = (seq, (stop + toward) * CORES + core)
    outward = (seq, (stop - toward) * CORES + core)
    sibling = (seq, stop * CORES + 1 - core)
    host = far >= 1 if fold else True

    def remote(source, target, send, receive, device):
        return pltpu.make_async_remote_copy(
            src_ref=source, dst_ref=target, send_sem=send, recv_sem=receive,
            device_id=device, device_id_type=MESH)

    def send(condition, make):
        when(condition, lambda: make().start())

    def origin(i):
        return jnp.where(far >= i, stop - i * toward, stop + (i - far) * toward)

    def rows(start, size):
        return pl.ds(pl.multiple_of(start * size, size), size)

    def block(j, o, c):
        return gw.at[j, rows(o * CORES + c, depth), :]

    def w_inward(j, o):
        b = block(j, o, core)
        return remote(b, b, w_in.at[0], w_rx.at[j, o], inward)

    def w_outward(j, o):
        b = block(j, o, core)
        return remote(b, b, w_out.at[0], w_rx.at[j, o], outward)

    def w_across(j, o):
        b = block(j, o, core)
        return remote(b, b, w_sib.at[0], w_rx.at[j, S], sibling)

    def w_arrive(i, j):
        with jax.named_scope(f"w{i}_{j}"):
            w_arrive_body(i, j)

    def w_arrive_body(i, j):
        o = origin(i)

        def take():
            b = block(j, o, core)
            remote(b, b, w_sib.at[0], w_rx.at[j, o], sibling).wait_recv()

        when(host, take)
        if i <= S // 2 - 1:
            send(far >= i, lambda: w_inward(j, o))
        if not fold:
            send((far < i) & (far >= 1), lambda: w_outward(j, o))
        send(host, lambda: w_across(j, o))

    def w_own_in(condition, j):
        send(condition, lambda: w_inward(j, stop))

    def w_other_core(j):
        with jax.named_scope(f"wsib_{j}"):
            w_other_core_body(j)

    def w_other_core_body(j):
        def take():
            b = gw.at[j, pl.ds(0, S * depth), :]
            remote(b, b, w_sib.at[0], w_rx.at[j, S], sibling).wait_recv()

        when(host, take)

    per_part = plan.part_rows
    piece = plan.rows_out // per_part
    pw = plan.part_cols

    def n_cut(pc):
        return pl.ds(pc % per_part * piece, piece), pl.ds(pc // per_part * pw, pw)

    def n_source(o, pc, own):
        r, c = n_cut(pc)
        return wo.at[r, c] if own else gathered.at[o * CORES + core, r, c]

    def n_target(o, c, pc):
        r, cut = n_cut(pc)
        return gathered.at[o * CORES + c, r, cut]

    def n_copy(o, pc, own, sem, device):
        return remote(n_source(o, pc, own), n_target(o, core, pc),
                      sem.at[0], n_rx.at[o, pc], device)

    def n_across(i, pc):
        o = stop if i == 0 else origin(i)
        arrive = n_rx.at[S, pc] if i == S - 1 else n_rx.at[S + 1, i]
        return remote(n_source(o, pc, i == 0), n_target(o, core, pc), n_sib.at[0], arrive, sibling)

    def n_across_wait(i, pc=None):
        if i == S - 1:
            t = n_target(origin(i), 1 - core, pc)
            remote(t, t, n_sib.at[0], n_rx.at[S, pc], sibling).wait_recv()
        else:
            t = gathered.at[0]
            remote(t, t, n_sib.at[0], n_rx.at[S + 1, i], sibling).wait_recv()

    def n_own_in(condition, pc):
        send(condition, lambda: n_copy(stop, pc, True, n_in, inward))

    def n_wait(o, pc):
        t = n_target(o, core, pc)
        remote(t, t, n_sib.at[0], n_rx.at[o, pc], sibling).wait_recv()

    def n_arrive(i, pc, who=True):
        o = origin(i)

        def take():
            with jax.named_scope(f"n{i}_{pc}"):
                n_wait(o, pc)

        when(who, take)
        if i <= S // 2 - 1:
            send(both_true(who, far >= i), lambda: n_copy(o, pc, False, n_in, inward))
        send(both_true(who, (far < i) & (far >= 1)),
             lambda: n_copy(o, pc, False, n_out, outward))
        send(who, lambda: n_across(i, pc))

    barrier = pltpu.get_barrier_semaphore()

    def greet(device):
        pl.semaphore_signal(barrier, inc=1, device_id=device, device_id_type=MESH)

    for k in range(1, G):
        greet((flip(seq, k), fsdp))
    greet(sibling)
    greet(inward)
    pl.when(far >= 1)(lambda: greet(outward))

    mine = rows(fsdp, depth)
    for j in range(C):
        for d in range(G):
            if j == 0:
                kv = pl.ds(d * plan.local_heads // plan.group_heads * HEAD, HEAD)
                for side, w in enumerate((wk, wv)):
                    spot = pl.ds(d * cw + side * HEAD, HEAD)
                    pltpu.make_async_copy(w.at[:, kv], gw.at[0, mine, spot], w_loc.at[0]).start()
            else:
                part_of = pl.ds(d * lw + (j - 1) * cw, cw)
                pltpu.make_async_copy(
                    wq.at[:, part_of], gw.at[j, mine, pl.ds(d * cw, cw)], w_loc.at[j]).start()
    load = pltpu.make_async_copy(tokens, tok, x_loc.at[0])
    load.start()

    pl.semaphore_wait(barrier, G + 1 + (far + S // 2 - 1) // (S // 2))

    for j in range(C):
        own = gw.at[j, mine, :]
        pltpu.make_async_copy(own, own, w_loc.at[j]).wait()
        if j == 0:
            w_own_in(True, 0)
        elif j == 1:
            w_own_in(True, 1)
        if not fold:
            send(far >= 1, lambda j=j: w_outward(j, stop))
        send(host, lambda j=j: w_across(j, stop))
    for pc in range(PIECES):
        send(far >= 1, lambda pc=pc: n_copy(stop, pc, True, n_out, outward))

    load.wait()

    def norm_rows(i, carry):
        r = rows(i, 16)
        x = tok[r, :].astype(F32)
        mean = jnp.mean(x * x, axis=-1, keepdims=True)
        tok[r, :] = (x * lax.rsqrt(mean + 1e-05) * gain[...]).astype(BF16)
        return carry

    lax.fori_loop(0, count // 16, norm_rows, 0)

    def x_copy(k):
        d = flip(seq, k)
        return remote(tok.at[:, rows(d, width)], nrm.at[0, rows(seq, count), :],
                      x_tx.at[0], x_rx.at[k], (d, fsdp))

    own_x = pltpu.make_async_copy(
        tok.at[:, rows(seq, width)], nrm.at[0, rows(seq, count), :], x_loc.at[1])
    own_x.start()
    for k in range(1, G):
        send(True, lambda k=k: x_copy(k))

    def x_wait(k):
        if k == 0:
            own_x.wait()
        else:
            spot = nrm.at[0, rows(flip(seq, k), count), :]
            remote(spot, spot, x_tx.at[0], x_rx.at[k], sibling).wait_recv()

    def g_copy(k):
        r = rows(flip(seq, k), count)
        return remote(nrm.at[0, r, :], nrm.at[turns - 1, r, :], g_tx.at[0], g_rx.at[0], inward)

    guest = far < 1
    if fold:
        for k in range(G):
            pl.when(guest)(lambda k=k: x_wait(k))
            send(guest, lambda k=k: g_copy(k))
        for j in range(2, C):
            w_own_in(guest, j)
        for pc in range(PIECES):
            n_own_in(guest, pc)

    stages = len(orders(0, G))

    def project(j, low, high):
        with jax.named_scope(f"project_{j}"):
            project_body(j, low, high)

    def project_body(j, low, high):
        def step(i, carry):
            t, k = high - 1 - i // G, G - 1 - i % G
            slot = j % SLOTS
            acc = jnp.dot(nrm[t], gw[j, :, rows(flip(seq, k), cw)], preferred_element_type=F32)
            for u in range(PAIR):
                part[slot, t, u, k] = acc[:, u * HEAD:(u + 1) * HEAD].astype(BF16)
            for u in range(PAIR):
                bit = u + 1

                @pl.when((k // bit) % 2 == 1)
                def _(u=u, bit=bit):
                    n = (k // (2 * bit)) * bit + k % bit
                    for q in range(1, stages + 1):
                        if q < stages:
                            mark = orders(u, G)[q]
                            before = [b for b in orders(u, G)[1:q]]
                        else:
                            mark, before = 0, orders(u, G)[1:]
                        hit = True
                        for b in before:
                            hit = both_true(hit, (k // b) % 2 == 0)
                        if mark:
                            hit = both_true(hit, (k // mark) % 2 == 1)

                        @pl.when(hit)
                        def _(q=q):
                            remote(part.at[slot, t, u, k], recv.at[j, t, u, n], r_tx.at[j],
                                   r_rx.at[j, t, q - 1], (flip(seq, bit), fsdp)).start()

            return carry

        lax.fori_loop(0, (high - low) * G, step, 0)

    def alive(u, q):
        bits = orders(u, G)[:q]
        return [k for k in range(G) if not any(k & b for b in bits)]

    def landing(u, q, k):
        return sum(len(alive(u, p + 1)) for p in range(q)) + alive(u, q + 1).index(k)

    def goes(u, k):
        for q, b in enumerate(orders(u, G)):
            if k & b:
                return q
        return stages

    def r_wait(j, t, q):
        units = sum(goes(0, k) for k in range(G) if goes(0, k) == q)
        spot = recv.at[j, t, :, pl.ds(0, units)]
        remote(spot, spot, r_tx.at[j], r_rx.at[j, t, q - 1], sibling).wait_recv()

    def total(j, t, u, upto, k, store):
        tile = 128

        def step(i, carry):
            r = rows(i, tile)
            value = part[j % SLOTS, t, u, k, r, :].astype(F32)
            for q in range(upto):
                value = value + recv[j, t, u, landing(u, q, k), r, :].astype(F32)
            store(r, value.astype(BF16))
            return carry

        lax.fori_loop(0, length // tile, step, 0)

    def stage(j, t):
        with jax.named_scope(f"stage_{j}_{t}"):
            stage_body(j, t)

    def stage_body(j, t):
        for q in range(1, stages):
            r_wait(j, t, q)
            for u in range(PAIR):
                bit = orders(u, G)[q]
                for k in reversed(alive(u, q)):
                    if k & bit:
                        def put(r, value, u=u, k=k):
                            part[j % SLOTS, t, u, k, r, :] = value

                        total(j, t, u, q, k, put)
                        n = landing(u, q, k ^ bit)
                        remote(part.at[j % SLOTS, t, u, k], recv.at[j, t, u, n], r_tx.at[j],
                               r_rx.at[j, t, goes(u, k ^ bit) - 1], (flip(seq, bit), fsdp)).start()

    def ret_copy(j):
        return remote(ret.at[j], fin.at[j], ret_tx.at[0], ret_rx.at[j], outward)

    def settle(j, t):
        with jax.named_scope(f"settle_{j}_{t}"):
            settle_body(j, t)

    def settle_body(j, t):
        r_wait(j, t, stages)
        for u in range(PAIR):
            def put(r, value, u=u):
                if t:
                    ret[j, r, pl.ds(u * HEAD, HEAD)] = value
                else:
                    fin[j, r, pl.ds(u * HEAD, HEAD)] = value

            total(j, t, u, stages, 0, put)
        if t:
            ret_copy(j).start()

    def returned(j):
        if fold:
            @pl.when(guest)
            def _():
                with jax.named_scope(f"returned_{j}"):
                    remote(fin.at[j], fin.at[j], ret_tx.at[0], ret_rx.at[j], sibling).wait_recv()

    def sent(j):
        p = part.at[j % SLOTS, :, :, pl.ds(0, G - 1)]
        remote(p, p, r_tx.at[j], r_rx.at[j, 0, 0], sibling).wait_send()

    relayed = G == 4
    near = [1, 2] if relayed else list(range(1, G))

    def h_spot(owner, j):
        return heads.at[:, rows(owner * (C - 1) + j - 1, cw)]

    def h_half(owner, j, u):
        return heads.at[:, rows((owner * (C - 1) + j - 1) * PAIR + u, HEAD)]

    def h_copy(j, k):
        spot = h_spot(seq, j)
        return remote(spot, spot, h_tx.at[0], h_rx.at[j, 0], (flip(seq, k), fsdp))

    def h_relay(j, u):
        came, then = orders(u, G)[:2]
        half = h_half(flip(seq, came), j, u)
        return remote(half, half, h_tx.at[0], h_rx.at[j, 1], (flip(seq, then), fsdp))

    def h_wait(j):
        with jax.named_scope(f"hwait_{j}"):
            spot = heads.at[:, pl.ds(0, len(near) * cw)]
            remote(spot, spot, h_tx.at[0], h_rx.at[j, 0], sibling).wait_recv()

    def relay(j):
        h_wait(j)
        if relayed:
            for u in range(PAIR):
                send(True, lambda u=u: h_relay(j, u))

    def h_last(j):
        if relayed:
            with jax.named_scope(f"hlast_{j}"):
                spot = h_spot(seq, j)
                remote(spot, spot, h_tx.at[0], h_rx.at[j, 1], sibling).wait_recv()

    def attend(j, condition=True):
        when(condition, lambda: mix(j))

    def mix(j):
        with jax.named_scope(f"attend_{j}"):
            mix_body(j)

    def mix_body(j):
        tile = 256

        def one_head(h, carry):
            column = rows(h, HEAD)
            for i in range(length // tile):
                seen = (i + 1) * tile
                q = fin[j, pl.ds(i * tile, tile), column]
                scores = lax.dot_general(
                    q, fin[0, pl.ds(0, seen), pl.ds(0, HEAD)],
                    (((1,), (1,)), ((), ())), preferred_element_type=F32) * (HEAD ** -0.5)
                row = lax.broadcasted_iota(jnp.int32, (tile, seen), 0) + i * tile
                col = lax.broadcasted_iota(jnp.int32, (tile, seen), 1)
                scores = jnp.where(row >= col, scores, F32(-1e30))
                top = jnp.max(scores, axis=-1, keepdims=True)
                weights = jnp.exp(scores - top)
                probs = weights * (1.0 / jnp.sum(weights, axis=-1, keepdims=True))
                mixed = jnp.dot(probs.astype(BF16), fin[0, pl.ds(0, seen), pl.ds(HEAD, HEAD)],
                                preferred_element_type=F32)
                spot = rows((seq * (C - 1) + j - 1) * PAIR + h, HEAD)
                heads[pl.ds(i * tile, tile), spot] = mixed.astype(BF16)
            return carry

        lax.fori_loop(0, PAIR, one_head, 0)
        for k in near:
            h_copy(j, k).start()

    def target(c, h):
        b = seq * plan.devices + c
        if not plan.flat:
            return out.at[b]
        return out.at[:, rows(b * plan.parts + h, pw)]

    def n_load(o, own, h, r, spot, sems):
        copies = []
        for n in range(CORES):
            c = core if n == 0 else 1 - core
            cut = pl.ds(h * pw, pw)
            source = wo.at[r, cut] if own and n == 0 else gathered.at[o * CORES + c, r, cut]
            where = spot.at[0, :, pl.ds(n * pw, pw)] if plan.flat else spot.at[n]
            copies.append(pltpu.make_async_copy(source, where, sems.at[h, n]))
        return copies

    def br_spot(o, h, n, r):
        if plan.flat:
            return br.at[o, h, 0, r, pl.ds(n * pw, pw)]
        return br.at[o, h, n, r, :]

    def br_send(o, h):
        for n in range(CORES):
            c = core if n == 0 else 1 - core
            for k in range(1, G):
                d = flip(seq, k)
                remote(br_spot(o, h, n, rows(d, count)), target(o * CORES + c, h),
                       b_tx.at[0], b_rx.at[0], (d, fsdp)).start()
            pltpu.make_async_copy(br_spot(o, h, n, rows(seq, count)), target(o * CORES + c, h),
                                  b_loc.at[0]).start()

    tile = 256
    ahead, late = (C - 2) * cw, cw

    def strips(i, o, own, start, size, place, sems):
        for h in range(plan.parts):
            for d in range(G):
                r = pl.ds(d * (C - 1) * cw + start, size)
                for copy in n_load(o, own, h, r, place(h, d), sems):
                    copy.start()

    def strips_wait(place, sems):
        for h in range(plan.parts):
            for n in range(CORES):
                spot = place(h)
                where = spot.at[0, :, pl.ds(n * pw, pw)] if plan.flat else spot.at[n]
                pltpu.make_async_copy(where, where, sems.at[h, n]).wait()

    def early_load(i):
        o = stop if i == 0 else origin(i)
        strips(i, o, i == 0, ahead, late,
               lambda h, d: nv_late.at[i % plan.kept, h, :, pl.ds(d * late, late), :], nl_sem)
        if ahead:
            strips(i, o, i == 0, 0, ahead,
                   lambda h, d: nv.at[h, :, pl.ds(d * ahead, ahead), :], nv_sem)

    def branch_early(i):
        with jax.named_scope(f"early_{i}"):
            strips_wait(lambda h: nv_late.at[i % plan.kept, h], nl_sem)
            if ahead:
                strips_wait(lambda h: nv.at[h, :, pl.ds(0, G * ahead), :], nv_sem)
                for h in range(plan.parts):
                    for unit in range(plan.units):
                        def step(t, carry, h=h, unit=unit):
                            r = rows(t, tile)
                            acc = None
                            for d in range(G):
                                p = jnp.dot(heads[r, pl.ds(d * (C - 1) * cw, ahead)],
                                            nv[h, unit, pl.ds(d * ahead, ahead), :],
                                            preferred_element_type=F32)
                                acc = p if acc is None else acc + p
                            br_acc[i % plan.kept, h, unit, r, :] = acc
                            return carry

                        lax.fori_loop(0, length // tile, step, 0)

    def branch(i):
        with jax.named_scope(f"branch_{i}"):
            o = stop if i == 0 else origin(i)
            for h in range(plan.parts):
                for unit in range(plan.units):
                    def step(t, carry, h=h, unit=unit):
                        r = rows(t, tile)
                        acc = br_acc[i % plan.kept, h, unit, r, :] if ahead else None
                        for d in range(G):
                            p = jnp.dot(heads[r, pl.ds(d * (C - 1) * cw + ahead, late)],
                                        nv_late[i % plan.kept, h, unit, pl.ds(d * late, late), :],
                                        preferred_element_type=F32)
                            acc = p if acc is None else acc + p
                        br[o, h, unit, r, :] = acc.astype(BF16)
                        return carry

                    lax.fori_loop(0, length // tile, step, 0)
                br_send(o, h)

    def branch_last(i):
        o = origin(i)

        def loads(pc):
            cut = pl.ds(pc % per_part * piece, piece)
            h = pc // per_part
            return n_load(o, False, h, cut, nv.at[h, :, cut, :], nl_sem if pc % 2 else nv_sem)

        begun = 0

        def begin(last):
            nonlocal begun
            while begun <= min(last, PIECES - 1):
                polls(i, begun, begun + 1)
                with jax.named_scope(f"nsib_{i}_{begun}"):
                    n_across_wait(i, begun)
                for copy in loads(begun):
                    copy.start()
                begun += 1

        for pc in range(PIECES):
            begin(pc + 1 if pc < PIECES - 2 else pc)
            h, q = pc // per_part, pc % per_part
            for copy in loads(pc):
                copy.wait()
            for unit in range(plan.units):
                def step(i, carry, h=h, q=q, unit=unit):
                    r = rows(i, tile)
                    cut = pl.ds(q * piece, piece)
                    acc = jnp.dot(heads[r, cut], nv[h, unit, cut, :], preferred_element_type=F32)
                    if q:
                        acc = acc + br_acc[plan.kept, h, unit, r, :]
                    if q < per_part - 1:
                        br_acc[plan.kept, h, unit, r, :] = acc
                    else:
                        br[o, h, unit, r, :] = acc.astype(BF16)
                    return carry

                lax.fori_loop(0, length // tile, step, 0)
            if q == per_part - 1:
                br_send(o, h)

    def both(action):
        for t in reversed(range(turns)):
            action(t)

    early = min(2, C)

    def both_early(action):
        for j in range(early):
            action(j, 1)

    def take_chunk(j):
        for i in range(2, S):
            w_arrive(i, j)
        w_other_core(j)

    for j in range(early):
        w_arrive(1, j)
    for pc in range(FILL):
        n_own_in(host, pc)
    if early < C:
        w_own_in(host, early)
    for j in range(early):
        take_chunk(j)
        if j == 0:
            when(host, lambda: [x_wait(k) for k in range(G)])
        when(host, lambda j=j: project(j, 0, 1))
        if j == 0:
            for pc in range(PIECES):
                send(True, lambda pc=pc: n_across(0, pc))

    def own_early():
        for j in range(early):
            stage(j, 0)
        for j in range(early):
            settle(j, 0)
        for j in range(1, early):
            mix(j)

    def guests_early():
        with jax.named_scope("gwait"):
            r = nrm.at[1]
            remote(r, r, g_tx.at[0], g_rx.at[0], sibling).wait_recv()
        for j in range(early):
            project(j, 1, 2)

    when(host, own_early)
    taken = []
    relays = [j for j in range(1, C)]

    def polls(i, first, last, role=None):
        for pc in range(first * PIECES // 8, min(last, 8) * PIECES // 8):
            for who, name in ((host, "host"), (guest, "guest")):
                if (i, pc, name) in taken or i >= S or role not in (None, name):
                    continue
                if name == "host" and role is None and (i, pc, "guest") not in taken:
                    taken.extend([(i, pc, "host"), (i, pc, "guest")])
                    n_arrive(i, pc)
                elif name == "host" or fold:
                    taken.append((i, pc, name))
                    n_arrive(i, pc, who)

    def gather(i):
        if i:
            polls(i, 0, 8)
        with jax.named_scope(f"nsib_{i}"):
            n_across_wait(i)

    def relay_to(j):
        while relays and relays[0] <= j:
            relay(relays.pop(0))

    def close(j):
        when(host, lambda: both(lambda t: settle(j, t)))
        returned(j)

    later = max(1, C - 1 - early)
    step_pieces = (PIECES - FILL) // later
    sent_in = FILL

    def fill(count):
        nonlocal sent_in
        for pc in range(sent_in, min(PIECES, sent_in + count)):
            n_own_in(host, pc)
        sent_in = min(PIECES, sent_in + count)

    def forward(j):
        if early <= j < C:
            w_arrive(1, j)
            if j + 1 < C:
                fill(step_pieces)
                w_own_in(host, j + 1)

    def attend_to(j):
        close(j)
        attend(j)

    polls(2, 0, 2, "host")
    if fold:
        when(host, guests_early)
    polls(2, 2, 4, "host")
    forward(early)
    if fold:
        when(host, lambda: both_early(stage))
        when(host, lambda: both_early(settle))
    forward(early + 1)
    if fold:
        polls(1, 0, 8, "guest")
        polls(2, 0, 4, "guest")
        for e in range(early):
            returned(e)
        for e in range(1, early):
            attend(e, guest)
    for j in range(early, C):
        take_chunk(j)
        last = j == C - 1
        if last:
            polls(1, 6, 8, "host")
            relay_to(j - 1)
        if j >= SLOTS:
            when(host, lambda j=j: sent(j - SLOTS))
        if last and fold:
            when(host, lambda j=j: project(j, 1, 2))
            polls(3, 0, 1, "host")
            when(host, lambda j=j: project(j, 0, 1))
        else:
            when(host, lambda j=j: project(j, 0, turns))
        if last:
            break
        relay_to(j - 2)
        when(host, lambda j=j: both(lambda t: stage(j, t)))
        if j == early:
            for e in range(early + 2, C):
                forward(e)
            fill(PIECES)
            polls(2, 4, 6, "host")
        if j == C - 2:
            polls(2, 6, 8, "host")
            polls(1, 0, 6, "host")
        attend_to(j)
        if j == early:
            polls(2, 4, 6, "guest")
    fill(PIECES)
    relay_to(C - 2)
    two_steps = fold and C > early
    if two_steps:
        polls(2, 0, 8, "guest")
        gather(0)
        early_load(0)
    polls(3, 0, 1, "host")
    for j in range(1, C - 1):
        h_last(j)
    if two_steps:
        branch_early(0)
        gather(1)
        early_load(1)
        polls(3, 1, 2, "host")
    if C > early:
        when(host, lambda: both(lambda t: stage(C - 1, t)))
    if two_steps:
        branch_early(1)
        gather(2)
        early_load(2)
        polls(3, 2, 3, "host")
    if C > early:
        attend_to(C - 1)
    if two_steps:
        polls(3, 3, 4, "host")
        branch_early(2)
        polls(3, 4, 5, "host")
        polls(3, 0, 3, "guest")
    relay_to(C - 1)
    polls(3, 5, 6, "host")
    polls(3, 3, 4, "guest")
    h_last(C - 1)
    polls(3, 6, 7, "host")
    polls(3, 4, 5, "guest")
    for i in range(S - 1):
        if not two_steps:
            gather(i)
            early_load(i)
            branch_early(i)
        branch(i)
    polls(3, 0, 8, "host")
    polls(3, 5, 6, "guest")
    if S > 1:
        branch_last(S - 1)

    def all_of(side):
        span = plan.devices * plan.cols_out
        return out.at[:, rows(side, span)] if plan.flat else out.at[rows(side, plan.devices)]

    def left(sem, count, spot):
        def wait():
            t = spot(count)
            remote(t, t, sem.at[0], r_rx.at[0, 0, 0], sibling).wait_send()

        return wait

    with jax.named_scope("sends"):
        def w_spot(n):
            return gw.at[:, pl.ds(0, n * depth), :]

        def n_spot(n):
            return gathered.at[pl.ds(0, n)]

        for v in range(S // 2):
            there = far == v
            pl.when(there)(left(n_in, 1 + v, n_spot))
            pl.when(there)(left(w_in, 1 + v, w_spot))
            if v:
                pl.when(there)(left(n_out, S - v, n_spot))
                if not fold:
                    pl.when(there)(left(w_out, S - v, w_spot))
        left(n_sib, S, n_spot)()
        when(host, left(w_sib, S, w_spot))
        left(x_tx, G - 1, lambda n: tok.at[:, pl.ds(0, n * width)])()
        left(h_tx, G - 1, lambda n: heads.at[:, pl.ds(0, n * lw)])()
        if fold:
            pl.when(guest)(left(g_tx, 0, lambda n: nrm.at[0]))
            pl.when(host)(left(ret_tx, 0, lambda n: ret))
        when(host, lambda: [sent(j) for j in range(max(0, C - SLOTS), C)])

    def others(first, n):
        if plan.flat:
            return out.at[:, pl.ds(first, n * plan.devices * plan.cols_out)]
        return out.at[pl.ds(first, n * plan.devices)]

    with jax.named_scope("bwait"):
        spot = others(0, G - 1)
        remote(spot, spot, b_tx.at[0], b_rx.at[0], sibling).wait()
        spot = others(0, 1)
        pltpu.make_async_copy(spot, spot, b_loc.at[0]).wait()


def body(tokens, norm_gain, w_query, key_weight, value_weight, w_out):
    group, devices = lax.axis_size("seq"), lax.axis_size("fsdp")
    plan = Plan(group, devices, tokens[0], w_query, key_weight, w_out)
    G, S, C, T = plan.group, plan.stops, plan.chunks, plan.turns
    length, cw = plan.length, plan.chunk
    unit_cols = plan.part_cols * CORES // plan.units
    any_space = pl.BlockSpec(memory_space=pl.ANY)
    dma = pltpu.SemaphoreType.DMA
    if plan.flat:
        out_shape = (plan.count, plan.features)
    else:
        out_shape = (G * devices, plan.count, plan.cols_out)
    stages = len(orders(0, G))
    branches, _ = pl.pallas_call(
        functools.partial(kernel, plan),
        out_shape=(
            jax.ShapeDtypeStruct(out_shape, BF16),
            jax.ShapeDtypeStruct((devices,) + w_out.shape, BF16),
        ),
        in_specs=[any_space, pl.BlockSpec(memory_space=pltpu.VMEM)] + [any_space] * 4,
        out_specs=(any_space, any_space),
        scratch_shapes=[
            pltpu.VMEM((plan.count, plan.features), BF16),
            pltpu.VMEM((C, plan.width, G * cw), BF16),
            pltpu.VMEM((T, length, plan.width), BF16),
            pltpu.VMEM((SLOTS, T, PAIR, G, length, HEAD), BF16),
            pltpu.VMEM((C, T, PAIR, G - 1, length, HEAD), BF16),
            pltpu.VMEM((C, length, cw), BF16),
            pltpu.VMEM((C if plan.fold else 1, length, cw), BF16),
            pltpu.VMEM((length, plan.rows_out), BF16),
            pltpu.VMEM((plan.parts, plan.units, plan.rows_out, unit_cols), BF16),
            pltpu.VMEM((plan.kept, plan.parts, plan.units, G * cw, unit_cols), BF16),
            pltpu.VMEM((S, plan.parts, plan.units, length, unit_cols), BF16),
            pltpu.VMEM((plan.kept + 1, plan.parts, plan.units, length, unit_cols), F32),
            dma((C, S + 1)), dma((1,)), dma((1,)), dma((1,)), dma((C,)),
            dma((S + 2, max(PIECES, S))), dma((1,)), dma((1,)), dma((1,)),
            dma((G,)), dma((1,)), dma((2,)), dma((1,)), dma((1,)),
            dma((C, T, stages)), dma((C,)), dma((C,)), dma((1,)),
            dma((C, 2)), dma((1,)), dma((1,)), dma((1,)), dma((1,)), dma((plan.parts, CORES)), dma((plan.parts, CORES)),
        ],
        compiler_params=pltpu.CompilerParams(
            collective_id=0, has_side_effects=True, vmem_limit_bytes=67043328),
    )(tokens[0], norm_gain[None], w_query, key_weight, value_weight, w_out)
    if not plan.flat:
        branches = jnp.transpose(branches, (1, 0, 2)).reshape(plan.count, plan.features)
    return tokens.astype(F32) + branches[None].astype(F32)


def solution(mesh):
    placed = (
        P("fsdp", "seq", None),
        P(),
        P(("seq", "fsdp"), None),
        P(("seq", "fsdp"), None),
        P(("seq", "fsdp"), None),
        P(None, ("seq", "fsdp")),
    )
    return jax.shard_map(
        body, mesh=mesh, in_specs=placed, out_specs=P("fsdp", "seq", None), check_vma=False
    )
```

```python
import functools

import jax
import jax.numpy as jnp
from jax import lax
from jax.experimental import pallas as pl
from jax.experimental.pallas import tpu as pltpu
from jax.sharding import PartitionSpec as P

HEAD = 128
CORES = 2
PAIR = 2
SLOTS = 2
PIECES = 8
FILL = 5
TAIL = 1
MESH = pl.DeviceIdType.MESH
F32, BF16 = jnp.float32, jnp.bfloat16


class Plan:
    def __init__(self, group, devices, tokens, w_query, key_weight, w_out):
        self.group, self.devices = group, devices
        self.stops = devices // CORES
        self.count, self.features = tokens.shape
        self.width = self.features // group
        self.depth = self.width // devices
        self.length = self.count * group
        self.rows_out, self.cols_out = w_out.shape
        heads = w_query.shape[1] // HEAD
        self.group_heads = heads // (key_weight.shape[1] // HEAD)
        self.local_heads = heads // group
        self.local_width = self.local_heads * HEAD
        self.chunk = PAIR * HEAD
        self.chunks = 1 + self.local_heads // PAIR
        self.flat = self.cols_out % HEAD == 0
        self.parts = self.cols_out // HEAD if self.flat else 1
        self.part_cols = self.cols_out // self.parts
        self.fold = self.stops == 4 and self.flat
        self.turns = 2 if self.fold else 1
        self.part_rows = PIECES // self.parts
        self.units = 1 if self.flat else CORES
        self.kept = self.stops - 1 if self.fold else 1


def when(condition, action):
    def run():
        action()

    if condition is True:
        run()
    else:
        pl.when(condition)(run)


def both_true(one, other):
    return other if one is True else one & other


def flip(index, mask):
    result, bit = index, 1
    while bit < 8:
        side = 1 - 2 * ((index // bit) % 2)
        result = result + ((mask // bit) % 2) * bit * side
        bit *= 2
    return result


def orders(turn, group):
    bits = []
    while 2 ** len(bits) < group:
        bits.append(2 ** len(bits))
    return bits[turn:] + bits[:turn]


def kernel(plan, tokens, gain, wq, wk, wv, wo, out, gathered,
           tok, gw, nrm, part, recv, fin, ret, heads, nv, nv_late, nl, br, br_acc,
           w_rx, w_in, w_out, w_sib, w_loc, n_rx, n_in, n_out, n_sib,
           x_rx, x_tx, x_loc, g_rx, g_tx, r_rx, r_tx, ret_rx, ret_tx,
           h_rx, h_tx, b_rx, b_tx, b_loc, nv_sem, nl_sem):
    G, S, C = plan.group, plan.stops, plan.chunks
    cw, depth, width, count = plan.chunk, plan.depth, plan.width, plan.count
    length, lw, fold, turns = plan.length, plan.local_width, plan.fold, plan.turns
    seq = lax.axis_index("seq")
    fsdp = lax.axis_index("fsdp")
    stop, core = fsdp // CORES, fsdp % CORES
    half = stop // (S // 2)
    toward = 1 - 2 * half
    far = half * (S - 1) + toward * stop
    inward = (seq, (stop + toward) * CORES + core)
    outward = (seq, (stop - toward) * CORES + core)
    sibling = (seq, stop * CORES + 1 - core)
    host = far >= 1 if fold else True

    def remote(source, target, send, receive, device):
        return pltpu.make_async_remote_copy(
            src_ref=source, dst_ref=target, send_sem=send, recv_sem=receive,
            device_id=device, device_id_type=MESH)

    def send(condition, make):
        when(condition, lambda: make().start())

    def origin(i):
        return jnp.where(far >= i, stop - i * toward, stop + (i - far) * toward)

    def rows(start, size):
        return pl.ds(pl.multiple_of(start * size, size), size)

    def block(j, o, c):
        return gw.at[j, rows(o * CORES + c, depth), :]

    def w_inward(j, o):
        b = block(j, o, core)
        return remote(b, b, w_in.at[0], w_rx.at[j, o], inward)

    def w_outward(j, o):
        b = block(j, o, core)
        return remote(b, b, w_out.at[0], w_rx.at[j, o], outward)

    def w_across(j, o):
        b = block(j, o, core)
        return remote(b, b, w_sib.at[0], w_rx.at[j, S], sibling)

    def w_arrive(i, j):
        with jax.named_scope(f"w{i}_{j}"):
            w_arrive_body(i, j)

    def w_arrive_body(i, j):
        o = origin(i)

        def take():
            b = block(j, o, core)
            remote(b, b, w_sib.at[0], w_rx.at[j, o], sibling).wait_recv()

        when(host, take)
        if i <= S // 2 - 1:
            send(far >= i, lambda: w_inward(j, o))
        if not fold:
            send((far < i) & (far >= 1), lambda: w_outward(j, o))
        send(host, lambda: w_across(j, o))

    def w_own_in(condition, j):
        send(condition, lambda: w_inward(j, stop))

    def w_other_core(j):
        with jax.named_scope(f"wsib_{j}"):
            w_other_core_body(j)

    def w_other_core_body(j):
        def take():
            b = gw.at[j, pl.ds(0, S * depth), :]
            remote(b, b, w_sib.at[0], w_rx.at[j, S], sibling).wait_recv()

        when(host, take)

    per_part = plan.part_rows
    piece = plan.rows_out // per_part
    pw = plan.part_cols

    def n_cut(pc):
        return pl.ds(pc % per_part * piece, piece), pl.ds(pc // per_part * pw, pw)

    def n_place(o, c, pc, last):
        r, cut = n_cut(pc)
        if last and fold:
            return nl.at[pc // per_part, r, rows(c, pw)]
        return gathered.at[o * CORES + c, r, cut]

    def n_source(o, pc, own, last):
        r, cut = n_cut(pc)
        return wo.at[r, cut] if own else n_place(o, core, pc, last)

    def n_copy(o, pc, own, sem, device, last=False, lands_last=False):
        return remote(n_source(o, pc, own, last), n_place(o, core, pc, lands_last),
                      sem.at[0], n_rx.at[o, pc], device)

    def n_across(i, pc):
        o = stop if i == 0 else origin(i)
        last = i == S - 1
        arrive = n_rx.at[S, pc] if last else n_rx.at[S + 1, i]
        return remote(n_source(o, pc, i == 0, last), n_place(o, core, pc, last),
                      n_sib.at[0], arrive, sibling)

    def n_across_wait(i, pc=None):
        if i == S - 1:
            t = n_place(origin(i), 1 - core, pc, True)
            remote(t, t, n_sib.at[0], n_rx.at[S, pc], sibling).wait_recv()
        else:
            t = gathered.at[0]
            remote(t, t, n_sib.at[0], n_rx.at[S + 1, i], sibling).wait_recv()

    def n_own_in(condition, pc):
        send(condition, lambda: n_copy(stop, pc, True, n_in, inward))

    def n_wait(i, pc):
        o = origin(i)
        t = n_place(o, core, pc, i == S - 1)
        remote(t, t, n_sib.at[0], n_rx.at[o, pc], sibling).wait_recv()

    def n_arrive(i, pc, who=True):
        o = origin(i)

        def take():
            with jax.named_scope(f"n{i}_{pc}"):
                n_wait(i, pc)

        when(who, take)
        if i <= S // 2 - 1:
            send(both_true(who, far >= i), lambda: n_copy(o, pc, False, n_in, inward, False, True))
        send(both_true(who, (far < i) & (far >= 1)),
             lambda: n_copy(o, pc, False, n_out, outward, i == S - 1, i == S - 1))
        send(who, lambda: n_across(i, pc))

    barrier = pltpu.get_barrier_semaphore()

    def greet(device):
        pl.semaphore_signal(barrier, inc=1, device_id=device, device_id_type=MESH)

    for k in range(1, G):
        greet((flip(seq, k), fsdp))
    greet(sibling)
    greet(inward)
    pl.when(far >= 1)(lambda: greet(outward))

    mine = rows(fsdp, depth)
    for j in range(C):
        for d in range(G):
            if j == 0:
                kv = pl.ds(d * plan.local_heads // plan.group_heads * HEAD, HEAD)
                for side, w in enumerate((wk, wv)):
                    spot = pl.ds(d * cw + side * HEAD, HEAD)
                    pltpu.make_async_copy(w.at[:, kv], gw.at[0, mine, spot], w_loc.at[0]).start()
            else:
                part_of = pl.ds(d * lw + (j - 1) * cw, cw)
                pltpu.make_async_copy(
                    wq.at[:, part_of], gw.at[j, mine, pl.ds(d * cw, cw)], w_loc.at[j]).start()
    load = pltpu.make_async_copy(tokens, tok, x_loc.at[0])
    load.start()

    pl.semaphore_wait(barrier, G + 1 + (far + S // 2 - 1) // (S // 2))

    for j in range(C):
        own = gw.at[j, mine, :]
        pltpu.make_async_copy(own, own, w_loc.at[j]).wait()
        if j == 0:
            w_own_in(True, 0)
        elif j == 1:
            w_own_in(True, 1)
        if not fold:
            send(far >= 1, lambda j=j: w_outward(j, stop))
        send(host, lambda j=j: w_across(j, stop))
    for pc in range(PIECES):
        send(far >= 1, lambda pc=pc: n_copy(stop, pc, True, n_out, outward))

    load.wait()

    def norm_rows(i, carry):
        r = rows(i, 16)
        x = tok[r, :].astype(F32)
        mean = jnp.mean(x * x, axis=-1, keepdims=True)
        tok[r, :] = (x * lax.rsqrt(mean + 1e-05) * gain[...]).astype(BF16)
        return carry

    lax.fori_loop(0, count // 16, norm_rows, 0)

    def x_copy(k):
        d = flip(seq, k)
        return remote(tok.at[:, rows(d, width)], nrm.at[0, rows(seq, count), :],
                      x_tx.at[0], x_rx.at[k], (d, fsdp))

    own_x = pltpu.make_async_copy(
        tok.at[:, rows(seq, width)], nrm.at[0, rows(seq, count), :], x_loc.at[1])
    own_x.start()
    for k in range(1, G):
        send(True, lambda k=k: x_copy(k))

    def x_wait(k):
        if k == 0:
            own_x.wait()
        else:
            spot = nrm.at[0, rows(flip(seq, k), count), :]
            remote(spot, spot, x_tx.at[0], x_rx.at[k], sibling).wait_recv()

    def g_copy(k):
        r = rows(flip(seq, k), count)
        return remote(nrm.at[0, r, :], nrm.at[turns - 1, r, :], g_tx.at[0], g_rx.at[0], inward)

    guest = far < 1
    if fold:
        for k in range(G):
            pl.when(guest)(lambda k=k: x_wait(k))
            send(guest, lambda k=k: g_copy(k))
        for j in range(2, C):
            w_own_in(guest, j)
        for pc in range(PIECES):
            n_own_in(guest, pc)

    stages = len(orders(0, G))

    def project(j, low, high):
        with jax.named_scope(f"project_{j}"):
            project_body(j, low, high)

    def project_body(j, low, high):
        def step(i, carry):
            t, k = high - 1 - i // G, G - 1 - i % G
            slot = j % SLOTS
            acc = jnp.dot(nrm[t], gw[j, :, rows(flip(seq, k), cw)], preferred_element_type=F32)
            for u in range(PAIR):
                part[slot, t, u, k] = acc[:, u * HEAD:(u + 1) * HEAD].astype(BF16)
            for u in range(PAIR):
                bit = u + 1

                @pl.when((k // bit) % 2 == 1)
                def _(u=u, bit=bit):
                    n = (k // (2 * bit)) * bit + k % bit
                    for q in range(1, stages + 1):
                        if q < stages:
                            mark = orders(u, G)[q]
                            before = [b for b in orders(u, G)[1:q]]
                        else:
                            mark, before = 0, orders(u, G)[1:]
                        hit = True
                        for b in before:
                            hit = both_true(hit, (k // b) % 2 == 0)
                        if mark:
                            hit = both_true(hit, (k // mark) % 2 == 1)

                        @pl.when(hit)
                        def _(q=q):
                            remote(part.at[slot, t, u, k], recv.at[j, t, u, n], r_tx.at[j],
                                   r_rx.at[j, t, q - 1], (flip(seq, bit), fsdp)).start()

            return carry

        lax.fori_loop(0, (high - low) * G, step, 0)

    def alive(u, q):
        bits = orders(u, G)[:q]
        return [k for k in range(G) if not any(k & b for b in bits)]

    def landing(u, q, k):
        return sum(len(alive(u, p + 1)) for p in range(q)) + alive(u, q + 1).index(k)

    def goes(u, k):
        for q, b in enumerate(orders(u, G)):
            if k & b:
                return q
        return stages

    def r_wait(j, t, q):
        units = sum(goes(0, k) for k in range(G) if goes(0, k) == q)
        spot = recv.at[j, t, :, pl.ds(0, units)]
        remote(spot, spot, r_tx.at[j], r_rx.at[j, t, q - 1], sibling).wait_recv()

    def total(j, t, u, upto, k, store):
        tile = 128

        def step(i, carry):
            r = rows(i, tile)
            value = part[j % SLOTS, t, u, k, r, :].astype(F32)
            for q in range(upto):
                value = value + recv[j, t, u, landing(u, q, k), r, :].astype(F32)
            store(r, value.astype(BF16))
            return carry

        lax.fori_loop(0, length // tile, step, 0)

    def stage(j, t):
        with jax.named_scope(f"stage_{j}_{t}"):
            stage_body(j, t)

    def stage_body(j, t):
        for q in range(1, stages):
            r_wait(j, t, q)
            for u in range(PAIR):
                bit = orders(u, G)[q]
                for k in reversed(alive(u, q)):
                    if k & bit:
                        def put(r, value, u=u, k=k):
                            part[j % SLOTS, t, u, k, r, :] = value

                        total(j, t, u, q, k, put)
                        n = landing(u, q, k ^ bit)
                        remote(part.at[j % SLOTS, t, u, k], recv.at[j, t, u, n], r_tx.at[j],
                               r_rx.at[j, t, goes(u, k ^ bit) - 1], (flip(seq, bit), fsdp)).start()

    def ret_copy(j):
        return remote(ret.at[j], fin.at[j], ret_tx.at[0], ret_rx.at[j], outward)

    def settle(j, t):
        with jax.named_scope(f"settle_{j}_{t}"):
            settle_body(j, t)

    def settle_body(j, t):
        r_wait(j, t, stages)
        for u in range(PAIR):
            def put(r, value, u=u):
                if t:
                    ret[j, r, pl.ds(u * HEAD, HEAD)] = value
                else:
                    fin[j, r, pl.ds(u * HEAD, HEAD)] = value

            total(j, t, u, stages, 0, put)
        if t:
            ret_copy(j).start()

    def returned(j):
        if fold:
            @pl.when(guest)
            def _():
                with jax.named_scope(f"returned_{j}"):
                    remote(fin.at[j], fin.at[j], ret_tx.at[0], ret_rx.at[j], sibling).wait_recv()

    def sent(j):
        p = part.at[j % SLOTS, :, :, pl.ds(0, G - 1)]
        remote(p, p, r_tx.at[j], r_rx.at[j, 0, 0], sibling).wait_send()

    relayed = G == 4
    near = [1, 2] if relayed else list(range(1, G))

    def h_spot(owner, j):
        return heads.at[:, rows(owner * (C - 1) + j - 1, cw)]

    def h_half(owner, j, u):
        return heads.at[:, rows((owner * (C - 1) + j - 1) * PAIR + u, HEAD)]

    def h_copy(j, k):
        spot = h_spot(seq, j)
        return remote(spot, spot, h_tx.at[0], h_rx.at[j, 0], (flip(seq, k), fsdp))

    def h_relay(j, u):
        came, then = orders(u, G)[:2]
        half = h_half(flip(seq, came), j, u)
        return remote(half, half, h_tx.at[0], h_rx.at[j, 1], (flip(seq, then), fsdp))

    def h_wait(j):
        with jax.named_scope(f"hwait_{j}"):
            spot = heads.at[:, pl.ds(0, len(near) * cw)]
            remote(spot, spot, h_tx.at[0], h_rx.at[j, 0], sibling).wait_recv()

    def relay(j):
        h_wait(j)
        if relayed:
            for u in range(PAIR):
                send(True, lambda u=u: h_relay(j, u))

    def h_last(j):
        if relayed:
            with jax.named_scope(f"hlast_{j}"):
                spot = h_spot(seq, j)
                remote(spot, spot, h_tx.at[0], h_rx.at[j, 1], sibling).wait_recv()

    def attend(j, condition=True):
        when(condition, lambda: mix(j))

    def mix(j):
        with jax.named_scope(f"attend_{j}"):
            mix_body(j)

    def mix_body(j):
        tile = 256

        def one_head(h, carry):
            column = rows(h, HEAD)
            for i in range(length // tile):
                seen = (i + 1) * tile
                q = fin[j, pl.ds(i * tile, tile), column]
                scores = lax.dot_general(
                    q, fin[0, pl.ds(0, seen), pl.ds(0, HEAD)],
                    (((1,), (1,)), ((), ())), preferred_element_type=F32) * (HEAD ** -0.5)
                row = lax.broadcasted_iota(jnp.int32, (tile, seen), 0) + i * tile
                col = lax.broadcasted_iota(jnp.int32, (tile, seen), 1)
                scores = jnp.where(row >= col, scores, F32(-1e30))
                top = jnp.max(scores, axis=-1, keepdims=True)
                weights = jnp.exp(scores - top)
                probs = weights * (1.0 / jnp.sum(weights, axis=-1, keepdims=True))
                mixed = jnp.dot(probs.astype(BF16), fin[0, pl.ds(0, seen), pl.ds(HEAD, HEAD)],
                                preferred_element_type=F32)
                spot = rows((seq * (C - 1) + j - 1) * PAIR + h, HEAD)
                heads[pl.ds(i * tile, tile), spot] = mixed.astype(BF16)
            return carry

        lax.fori_loop(0, PAIR, one_head, 0)
        for k in near:
            h_copy(j, k).start()

    def target(c, h):
        b = seq * plan.devices + c
        if not plan.flat:
            return out.at[b]
        return out.at[:, rows(b * plan.parts + h, pw)]

    def n_load(o, own, h, r, spot, sems):
        copies = []
        for n in range(CORES):
            c = core if n == 0 else 1 - core
            cut = pl.ds(h * pw, pw)
            source = wo.at[r, cut] if own and n == 0 else gathered.at[o * CORES + c, r, cut]
            where = spot.at[0, :, pl.ds(n * pw, pw)] if plan.flat else spot.at[n]
            copies.append(pltpu.make_async_copy(source, where, sems.at[h, n]))
        return copies

    def br_spot(o, h, n, r):
        if plan.flat:
            return br.at[o, h, 0, r, pl.ds(n * pw, pw)]
        return br.at[o, h, n, r, :]

    def br_send(o, h, ordered=False):
        for n in range(CORES):
            c = n if ordered else (core if n == 0 else 1 - core)
            for k in range(1, G):
                d = flip(seq, k)
                remote(br_spot(o, h, n, rows(d, count)), target(o * CORES + c, h),
                       b_tx.at[0], b_rx.at[0], (d, fsdp)).start()
            pltpu.make_async_copy(br_spot(o, h, n, rows(seq, count)), target(o * CORES + c, h),
                                  b_loc.at[0]).start()

    tile = 256
    ahead, late = (C - 2) * cw, cw

    def strips(i, o, own, start, size, place, sems):
        for h in range(plan.parts):
            for d in range(G):
                r = pl.ds(d * (C - 1) * cw + start, size)
                for copy in n_load(o, own, h, r, place(h, d), sems):
                    copy.start()

    def strips_wait(place, sems):
        for h in range(plan.parts):
            for n in range(CORES):
                spot = place(h)
                where = spot.at[0, :, pl.ds(n * pw, pw)] if plan.flat else spot.at[n]
                pltpu.make_async_copy(where, where, sems.at[h, n]).wait()

    def early_load(i):
        o = stop if i == 0 else origin(i)
        strips(i, o, i == 0, ahead, late,
               lambda h, d: nv_late.at[i % plan.kept, h, :, pl.ds(d * late, late), :], nl_sem)
        if ahead:
            strips(i, o, i == 0, 0, ahead,
                   lambda h, d: nv.at[h, :, pl.ds(d * ahead, ahead), :], nv_sem)

    def branch_early(i):
        with jax.named_scope(f"early_{i}"):
            strips_wait(lambda h: nv_late.at[i % plan.kept, h], nl_sem)
            if ahead:
                strips_wait(lambda h: nv.at[h, :, pl.ds(0, G * ahead), :], nv_sem)
                for h in range(plan.parts):
                    for unit in range(plan.units):
                        def step(t, carry, h=h, unit=unit):
                            r = rows(t, tile)
                            acc = None
                            for d in range(G):
                                p = jnp.dot(heads[r, pl.ds(d * (C - 1) * cw, ahead)],
                                            nv[h, unit, pl.ds(d * ahead, ahead), :],
                                            preferred_element_type=F32)
                                acc = p if acc is None else acc + p
                            br_acc[i % plan.kept, h, unit, r, :] = acc
                            return carry

                        lax.fori_loop(0, length // tile, step, 0)

    def branch(i):
        with jax.named_scope(f"branch_{i}"):
            o = stop if i == 0 else origin(i)
            for h in range(plan.parts):
                for unit in range(plan.units):
                    def step(t, carry, h=h, unit=unit):
                        r = rows(t, tile)
                        acc = br_acc[i % plan.kept, h, unit, r, :] if ahead else None
                        for d in range(G):
                            p = jnp.dot(heads[r, pl.ds(d * (C - 1) * cw + ahead, late)],
                                        nv_late[i % plan.kept, h, unit, pl.ds(d * late, late), :],
                                        preferred_element_type=F32)
                            acc = p if acc is None else acc + p
                        br[o, h, unit, r, :] = acc.astype(BF16)
                        return carry

                    lax.fori_loop(0, length // tile, step, 0)
                br_send(o, h)

    def branch_last(i):
        o = origin(i)

        def loads(pc):
            cut = pl.ds(pc % per_part * piece, piece)
            h = pc // per_part
            return n_load(o, False, h, cut, nv.at[h, :, cut, :], nl_sem if pc % 2 else nv_sem)

        begun = 0

        def begin(last):
            nonlocal begun
            while begun <= min(last, PIECES - 1):
                polls(i, begun, begun + 1)
                with jax.named_scope(f"nsib_{i}_{begun}"):
                    n_across_wait(i, begun)
                if not fold:
                    for copy in loads(begun):
                        copy.start()
                begun += 1

        for pc in range(PIECES):
            begin(pc + 1 if pc < PIECES - 2 else pc)
            h, q = pc // per_part, pc % per_part
            if not fold:
                for copy in loads(pc):
                    copy.wait()
            for unit in range(plan.units):
                def step(i, carry, h=h, q=q, unit=unit):
                    r = rows(i, tile)
                    cut = pl.ds(q * piece, piece)
                    w = nl[h, cut, :] if fold else nv[h, unit, cut, :]
                    acc = jnp.dot(heads[r, cut], w, preferred_element_type=F32)
                    if q:
                        acc = acc + br_acc[plan.kept, h, unit, r, :]
                    if q < per_part - 1:
                        br_acc[plan.kept, h, unit, r, :] = acc
                    else:
                        br[o, h, unit, r, :] = acc.astype(BF16)
                    return carry

                lax.fori_loop(0, length // tile, step, 0)
            if q == per_part - 1:
                br_send(o, h, fold)

    def both(action):
        for t in reversed(range(turns)):
            action(t)

    early = min(2, C)

    def both_early(action):
        for j in range(early):
            action(j, 1)

    def take_chunk(j):
        for i in range(2, S):
            w_arrive(i, j)
        w_other_core(j)

    for j in range(early):
        w_arrive(1, j)
    for pc in range(FILL):
        n_own_in(host, pc)
    if early < C:
        w_own_in(host, early)
    for j in range(early):
        take_chunk(j)
        if j == 0:
            when(host, lambda: [x_wait(k) for k in range(G)])
        when(host, lambda j=j: project(j, 0, 1))
        if j == 0:
            for pc in range(PIECES):
                send(True, lambda pc=pc: n_across(0, pc))

    def own_early():
        for j in range(early):
            stage(j, 0)
        for j in range(early):
            settle(j, 0)
        for j in range(1, early):
            mix(j)

    def guests_early():
        with jax.named_scope("gwait"):
            r = nrm.at[1]
            remote(r, r, g_tx.at[0], g_rx.at[0], sibling).wait_recv()
        for j in range(early):
            project(j, 1, 2)

    when(host, own_early)
    taken = []
    relays = [j for j in range(1, C)]

    def polls(i, first, last, role=None):
        for pc in range(first * PIECES // 8, min(last, 8) * PIECES // 8):
            for who, name in ((host, "host"), (guest, "guest")):
                if (i, pc, name) in taken or i >= S or role not in (None, name):
                    continue
                if name == "host" and role is None and (i, pc, "guest") not in taken:
                    taken.extend([(i, pc, "host"), (i, pc, "guest")])
                    n_arrive(i, pc)
                elif name == "host" or fold:
                    taken.append((i, pc, name))
                    n_arrive(i, pc, who)

    def gather(i):
        if i:
            polls(i, 0, 8)
        with jax.named_scope(f"nsib_{i}"):
            n_across_wait(i)

    def relay_to(j):
        while relays and relays[0] <= j:
            relay(relays.pop(0))

    def close(j):
        when(host, lambda: both(lambda t: settle(j, t)))
        returned(j)

    sent_in = FILL

    def fill(count):
        nonlocal sent_in
        for pc in range(sent_in, min(PIECES, sent_in + count)):
            n_own_in(host, pc)
        sent_in = min(PIECES, sent_in + count)

    def forward(j):
        if early <= j < C:
            w_arrive(1, j)
            if j + 1 < C:
                fill((PIECES - TAIL - sent_in) // (C - 1 - j))
                w_own_in(host, j + 1)

    def attend_to(j):
        close(j)
        attend(j)

    polls(2, 0, 2, "host")
    if fold:
        when(host, guests_early)
    polls(2, 2, 4, "host")
    forward(early)
    if fold:
        when(host, lambda: both_early(stage))
        when(host, lambda: both_early(settle))
    forward(early + 1)
    if fold:
        polls(1, 0, 8, "guest")
        polls(2, 0, 4, "guest")
        for e in range(early):
            returned(e)
        for e in range(1, early):
            attend(e, guest)
    for j in range(early, C):
        take_chunk(j)
        last = j == C - 1
        if last:
            polls(1, 6, 8, "host")
            relay_to(j - 1)
            if fold:
                polls(2, 0, 8 - TAIL, "guest")
                gather(0)
                early_load(0)
        if j >= SLOTS:
            when(host, lambda j=j: sent(j - SLOTS))
        if last and fold:
            when(host, lambda j=j: project(j, 1, 2))
            polls(2, 8 - TAIL, 8, "host")
            when(host, lambda j=j: project(j, 0, 1))
        else:
            when(host, lambda j=j: project(j, 0, turns))
        if last:
            break
        relay_to(j - 2)
        when(host, lambda j=j: both(lambda t: stage(j, t)))
        if j == early:
            for e in range(early + 2, C):
                forward(e)
            fill(PIECES)
            polls(2, 4, 6, "host")
        if j == C - 2:
            polls(2, 6, 8 - TAIL, "host")
            polls(1, 0, 6, "host")
        attend_to(j)
        if j == early:
            polls(2, 4, 6, "guest")
    fill(PIECES)
    relay_to(C - 2)
    two_steps = fold and C > early
    polls(3, 0, 1, "host")
    for j in range(1, C - 1):
        h_last(j)
    if two_steps:
        branch_early(0)
        gather(1)
        early_load(1)
    if C > early:
        when(host, lambda: both(lambda t: stage(C - 1, t)))
    if two_steps:
        polls(3, 1, 2, "host")
        branch_early(1)
        gather(2)
        early_load(2)
    if C > early:
        close(C - 1)
        polls(3, 2, 3, "host")
        attend(C - 1)
    if two_steps:
        polls(3, 3, 4, "host")
        branch_early(2)
        polls(3, 4, 5, "host")
        polls(3, 0, 3, "guest")
    relay_to(C - 1)
    polls(3, 5, 6, "host")
    h_last(C - 1)
    polls(3, 6, 7, "host")
    for i in range(S - 1):
        if not two_steps:
            gather(i)
            early_load(i)
            branch_early(i)
        branch(i)
    polls(3, 0, 8, "host")
    polls(3, 3, 6, "guest")
    if S > 1:
        branch_last(S - 1)

    def all_of(side):
        span = plan.devices * plan.cols_out
        return out.at[:, rows(side, span)] if plan.flat else out.at[rows(side, plan.devices)]

    def left(sem, count, spot):
        def wait():
            t = spot(count)
            remote(t, t, sem.at[0], r_rx.at[0, 0, 0], sibling).wait_send()

        return wait

    with jax.named_scope("sends"):
        def w_spot(n):
            return gw.at[:, pl.ds(0, n * depth), :]

        def n_spot(n):
            return gathered.at[pl.ds(0, n)]

        for v in range(S // 2):
            there = far == v
            pl.when(there)(left(n_in, 1 + v, n_spot))
            pl.when(there)(left(w_in, 1 + v, w_spot))
            if v:
                pl.when(there)(left(n_out, S - v, n_spot))
                if not fold:
                    pl.when(there)(left(w_out, S - v, w_spot))
        left(n_sib, S, n_spot)()
        when(host, left(w_sib, S, w_spot))
        left(x_tx, G - 1, lambda n: tok.at[:, pl.ds(0, n * width)])()
        left(h_tx, G - 1, lambda n: heads.at[:, pl.ds(0, n * lw)])()
        if fold:
            pl.when(guest)(left(g_tx, 0, lambda n: nrm.at[0]))
            pl.when(host)(left(ret_tx, 0, lambda n: ret))
        when(host, lambda: [sent(j) for j in range(max(0, C - SLOTS), C)])

    def others(first, n):
        if plan.flat:
            return out.at[:, pl.ds(first, n * plan.devices * plan.cols_out)]
        return out.at[pl.ds(first, n * plan.devices)]

    with jax.named_scope("bwait"):
        spot = others(0, G - 1)
        remote(spot, spot, b_tx.at[0], b_rx.at[0], sibling).wait()
        spot = others(0, 1)
        pltpu.make_async_copy(spot, spot, b_loc.at[0]).wait()


def body(tokens, norm_gain, w_query, key_weight, value_weight, w_out):
    group, devices = lax.axis_size("seq"), lax.axis_size("fsdp")
    plan = Plan(group, devices, tokens[0], w_query, key_weight, w_out)
    G, S, C, T = plan.group, plan.stops, plan.chunks, plan.turns
    length, cw = plan.length, plan.chunk
    unit_cols = plan.part_cols * CORES // plan.units
    any_space = pl.BlockSpec(memory_space=pl.ANY)
    dma = pltpu.SemaphoreType.DMA
    if plan.flat:
        out_shape = (plan.count, plan.features)
    else:
        out_shape = (G * devices, plan.count, plan.cols_out)
    stages = len(orders(0, G))
    nv_rows = max(16, G * (C - 2) * cw) if plan.fold else plan.rows_out
    branches, _ = pl.pallas_call(
        functools.partial(kernel, plan),
        out_shape=(
            jax.ShapeDtypeStruct(out_shape, BF16),
            jax.ShapeDtypeStruct((devices,) + w_out.shape, BF16),
        ),
        in_specs=[any_space, pl.BlockSpec(memory_space=pltpu.VMEM)] + [any_space] * 4,
        out_specs=(any_space, any_space),
        scratch_shapes=[
            pltpu.VMEM((plan.count, plan.features), BF16),
            pltpu.VMEM((C, plan.width, G * cw), BF16),
            pltpu.VMEM((T, length, plan.width), BF16),
            pltpu.VMEM((SLOTS, T, PAIR, G, length, HEAD), BF16),
            pltpu.VMEM((C, T, PAIR, G - 1, length, HEAD), BF16),
            pltpu.VMEM((C, length, cw), BF16),
            pltpu.VMEM((C if plan.fold else 1, length, cw), BF16),
            pltpu.VMEM((length, plan.rows_out), BF16),
            pltpu.VMEM((plan.parts, plan.units, nv_rows, unit_cols), BF16),
            pltpu.VMEM((plan.kept, plan.parts, plan.units, G * cw, unit_cols), BF16),
            pltpu.VMEM((plan.parts, plan.rows_out if plan.fold else 16, unit_cols), BF16),
            pltpu.VMEM((S, plan.parts, plan.units, length, unit_cols), BF16),
            pltpu.VMEM((plan.kept + 1, plan.parts, plan.units, length, unit_cols), F32),
            dma((C, S + 1)), dma((1,)), dma((1,)), dma((1,)), dma((C,)),
            dma((S + 2, max(PIECES, S))), dma((1,)), dma((1,)), dma((1,)),
            dma((G,)), dma((1,)), dma((2,)), dma((1,)), dma((1,)),
            dma((C, T, stages)), dma((C,)), dma((C,)), dma((1,)),
            dma((C, 2)), dma((1,)), dma((1,)), dma((1,)), dma((1,)), dma((plan.parts, CORES)), dma((plan.parts, CORES)),
        ],
        compiler_params=pltpu.CompilerParams(
            collective_id=0, has_side_effects=True, vmem_limit_bytes=67043328),
    )(tokens[0], norm_gain[None], w_query, key_weight, value_weight, w_out)
    if not plan.flat:
        branches = jnp.transpose(branches, (1, 0, 2)).reshape(plan.count, plan.features)
    return tokens.astype(F32) + branches[None].astype(F32)


def solution(mesh):
    placed = (
        P("fsdp", "seq", None),
        P(),
        P(("seq", "fsdp"), None),
        P(("seq", "fsdp"), None),
        P(("seq", "fsdp"), None),
        P(None, ("seq", "fsdp")),
    )
    return jax.shard_map(
        body, mesh=mesh, in_specs=placed, out_specs=P("fsdp", "seq", None), check_vma=False
    )
```

```python
import functools

import jax
import jax.numpy as jnp
from jax import lax
from jax.experimental import pallas as pl
from jax.experimental.pallas import tpu as pltpu
from jax.sharding import PartitionSpec as P

HEAD = 128
CORES = 2
PAIR = 2
SLOTS = 2
PIECES = 8
FILL = 5
TAIL = 1
MESH = pl.DeviceIdType.MESH
F32, BF16 = jnp.float32, jnp.bfloat16


class Plan:
    def __init__(self, group, devices, tokens, w_query, key_weight, w_out):
        self.group, self.devices = group, devices
        self.stops = devices // CORES
        self.count, self.features = tokens.shape
        self.width = self.features // group
        self.depth = self.width // devices
        self.length = self.count * group
        self.rows_out, self.cols_out = w_out.shape
        heads = w_query.shape[1] // HEAD
        self.group_heads = heads // (key_weight.shape[1] // HEAD)
        self.local_heads = heads // group
        self.local_width = self.local_heads * HEAD
        self.chunk = PAIR * HEAD
        self.chunks = 1 + self.local_heads // PAIR
        self.flat = self.cols_out % HEAD == 0
        self.parts = self.cols_out // HEAD if self.flat else 1
        self.part_cols = self.cols_out // self.parts
        self.fold = self.stops == 4 and self.flat
        self.turns = 2 if self.fold else 1
        self.part_rows = PIECES // self.parts
        self.units = 1 if self.flat else CORES
        self.kept = self.stops - 1 if self.fold else 1


def when(condition, action):
    def run():
        action()

    if condition is True:
        run()
    else:
        pl.when(condition)(run)


def both_true(one, other):
    return other if one is True else one & other


def flip(index, mask):
    result, bit = index, 1
    while bit < 8:
        side = 1 - 2 * ((index // bit) % 2)
        result = result + ((mask // bit) % 2) * bit * side
        bit *= 2
    return result


def orders(turn, group):
    bits = []
    while 2 ** len(bits) < group:
        bits.append(2 ** len(bits))
    return bits[turn:] + bits[:turn]


def kernel(plan, tokens, gain, wq, wk, wv, wo, out, gathered,
           tok, gw, nrm, part, recv, fin, ret, heads, nv, nv_late, nl, br, br_acc,
           w_rx, w_in, w_out, w_sib, w_loc, n_rx, n_in, n_out, n_sib,
           x_rx, x_tx, x_loc, g_rx, g_tx, r_rx, r_tx, ret_rx, ret_tx,
           h_rx, h_tx, b_rx, b_tx, b_loc, nv_sem, nl_sem):
    G, S, C = plan.group, plan.stops, plan.chunks
    cw, depth, width, count = plan.chunk, plan.depth, plan.width, plan.count
    length, lw, fold, turns = plan.length, plan.local_width, plan.fold, plan.turns
    seq = lax.axis_index("seq")
    fsdp = lax.axis_index("fsdp")
    stop, core = fsdp // CORES, fsdp % CORES
    half = stop // (S // 2)
    toward = 1 - 2 * half
    far = half * (S - 1) + toward * stop
    inward = (seq, (stop + toward) * CORES + core)
    outward = (seq, (stop - toward) * CORES + core)
    sibling = (seq, stop * CORES + 1 - core)
    host = far >= 1 if fold else True

    def remote(source, target, send, receive, device):
        return pltpu.make_async_remote_copy(
            src_ref=source, dst_ref=target, send_sem=send, recv_sem=receive,
            device_id=device, device_id_type=MESH)

    def send(condition, make):
        when(condition, lambda: make().start())

    def origin(i):
        return jnp.where(far >= i, stop - i * toward, stop + (i - far) * toward)

    def rows(start, size):
        return pl.ds(pl.multiple_of(start * size, size), size)

    def block(j, o, c):
        return gw.at[j, rows(o * CORES + c, depth), :]

    def w_inward(j, o):
        b = block(j, o, core)
        return remote(b, b, w_in.at[0], w_rx.at[j, o], inward)

    def w_outward(j, o):
        b = block(j, o, core)
        return remote(b, b, w_out.at[0], w_rx.at[j, o], outward)

    def w_across(j, o):
        b = block(j, o, core)
        return remote(b, b, w_sib.at[0], w_rx.at[j, S], sibling)

    def w_arrive(i, j):
        with jax.named_scope(f"w{i}_{j}"):
            w_arrive_body(i, j)

    def w_arrive_body(i, j):
        o = origin(i)

        def take():
            b = block(j, o, core)
            remote(b, b, w_sib.at[0], w_rx.at[j, o], sibling).wait_recv()

        when(host, take)
        if i <= S // 2 - 1:
            send(far >= i, lambda: w_inward(j, o))
        if not fold:
            send((far < i) & (far >= 1), lambda: w_outward(j, o))
        send(host, lambda: w_across(j, o))

    def w_own_in(condition, j):
        send(condition, lambda: w_inward(j, stop))

    def w_other_core(j):
        with jax.named_scope(f"wsib_{j}"):
            w_other_core_body(j)

    def w_other_core_body(j):
        def take():
            b = gw.at[j, pl.ds(0, S * depth), :]
            remote(b, b, w_sib.at[0], w_rx.at[j, S], sibling).wait_recv()

        when(host, take)

    per_part = plan.part_rows
    piece = plan.rows_out // per_part
    pw = plan.part_cols

    def n_cut(pc):
        return pl.ds(pc % per_part * piece, piece), pl.ds(pc // per_part * pw, pw)

    def n_place(o, c, pc, last):
        r, cut = n_cut(pc)
        if last and fold:
            return nl.at[pc // per_part, r, rows(c, pw)]
        return gathered.at[o * CORES + c, r, cut]

    def n_source(o, pc, own, last):
        r, cut = n_cut(pc)
        return wo.at[r, cut] if own else n_place(o, core, pc, last)

    def n_copy(o, pc, own, sem, device, last=False, lands_last=False):
        return remote(n_source(o, pc, own, last), n_place(o, core, pc, lands_last),
                      sem.at[0], n_rx.at[o, pc], device)

    def n_across(i, pc):
        o = stop if i == 0 else origin(i)
        last = i == S - 1
        arrive = n_rx.at[S, pc] if last else n_rx.at[S + 1, i]
        return remote(n_source(o, pc, i == 0, last), n_place(o, core, pc, last),
                      n_sib.at[0], arrive, sibling)

    def n_across_wait(i, pc=None):
        if i == S - 1:
            t = n_place(origin(i), 1 - core, pc, True)
            remote(t, t, n_sib.at[0], n_rx.at[S, pc], sibling).wait_recv()
        else:
            t = gathered.at[0]
            remote(t, t, n_sib.at[0], n_rx.at[S + 1, i], sibling).wait_recv()

    def n_own_in(condition, pc):
        send(condition, lambda: n_copy(stop, pc, True, n_in, inward))

    def n_wait(i, pc):
        o = origin(i)
        t = n_place(o, core, pc, i == S - 1)
        remote(t, t, n_sib.at[0], n_rx.at[o, pc], sibling).wait_recv()

    def n_arrive(i, pc, who=True):
        o = origin(i)

        def take():
            with jax.named_scope(f"n{i}_{pc}"):
                n_wait(i, pc)

        when(who, take)
        if i <= S // 2 - 1:
            send(both_true(who, far >= i), lambda: n_copy(o, pc, False, n_in, inward, False, True))
        send(both_true(who, (far < i) & (far >= 1)),
             lambda: n_copy(o, pc, False, n_out, outward, i == S - 1, i == S - 1))
        send(who, lambda: n_across(i, pc))

    barrier = pltpu.get_barrier_semaphore()

    def greet(device):
        pl.semaphore_signal(barrier, inc=1, device_id=device, device_id_type=MESH)

    for k in range(1, G):
        greet((flip(seq, k), fsdp))
    greet(sibling)
    greet(inward)
    pl.when(far >= 1)(lambda: greet(outward))

    mine = rows(fsdp, depth)
    for j in range(C):
        for d in range(G):
            if j == 0:
                kv = pl.ds(d * plan.local_heads // plan.group_heads * HEAD, HEAD)
                for side, w in enumerate((wk, wv)):
                    spot = pl.ds(d * cw + side * HEAD, HEAD)
                    pltpu.make_async_copy(w.at[:, kv], gw.at[0, mine, spot], w_loc.at[0]).start()
            else:
                part_of = pl.ds(d * lw + (j - 1) * cw, cw)
                pltpu.make_async_copy(
                    wq.at[:, part_of], gw.at[j, mine, pl.ds(d * cw, cw)], w_loc.at[j]).start()
    load = pltpu.make_async_copy(tokens, tok, x_loc.at[0])
    load.start()

    pl.semaphore_wait(barrier, G + 1 + (far + S // 2 - 1) // (S // 2))

    for j in range(C):
        own = gw.at[j, mine, :]
        pltpu.make_async_copy(own, own, w_loc.at[j]).wait()
        if j == 0:
            w_own_in(True, 0)
        elif j == 1:
            w_own_in(True, 1)
        if not fold:
            send(far >= 1, lambda j=j: w_outward(j, stop))
        send(host, lambda j=j: w_across(j, stop))
    for pc in range(PIECES):
        send(far >= 1, lambda pc=pc: n_copy(stop, pc, True, n_out, outward))

    load.wait()

    def norm_rows(i, carry):
        r = rows(i, 16)
        x = tok[r, :].astype(F32)
        mean = jnp.mean(x * x, axis=-1, keepdims=True)
        tok[r, :] = (x * lax.rsqrt(mean + 1e-05) * gain[...]).astype(BF16)
        return carry

    lax.fori_loop(0, count // 16, norm_rows, 0)

    def x_copy(k):
        d = flip(seq, k)
        return remote(tok.at[:, rows(d, width)], nrm.at[0, rows(seq, count), :],
                      x_tx.at[0], x_rx.at[k], (d, fsdp))

    own_x = pltpu.make_async_copy(
        tok.at[:, rows(seq, width)], nrm.at[0, rows(seq, count), :], x_loc.at[1])
    own_x.start()
    for k in range(1, G):
        send(True, lambda k=k: x_copy(k))

    def x_wait(k):
        if k == 0:
            own_x.wait()
        else:
            spot = nrm.at[0, rows(flip(seq, k), count), :]
            remote(spot, spot, x_tx.at[0], x_rx.at[k], sibling).wait_recv()

    def g_copy(k):
        r = rows(flip(seq, k), count)
        return remote(nrm.at[0, r, :], nrm.at[turns - 1, r, :], g_tx.at[0], g_rx.at[0], inward)

    guest = far < 1
    if fold:
        for k in range(G):
            pl.when(guest)(lambda k=k: x_wait(k))
            send(guest, lambda k=k: g_copy(k))
        for j in range(2, C):
            w_own_in(guest, j)
        for pc in range(PIECES):
            n_own_in(guest, pc)

    stages = len(orders(0, G))

    def project(j, low, high):
        with jax.named_scope(f"project_{j}"):
            project_body(j, low, high)

    def project_body(j, low, high):
        def step(i, carry):
            t, k = high - 1 - i // G, G - 1 - i % G
            slot = j % SLOTS
            acc = jnp.dot(nrm[t], gw[j, :, rows(flip(seq, k), cw)], preferred_element_type=F32)
            for u in range(PAIR):
                part[slot, t, u, k] = acc[:, u * HEAD:(u + 1) * HEAD].astype(BF16)
            for u in range(PAIR):
                bit = u + 1

                @pl.when((k // bit) % 2 == 1)
                def _(u=u, bit=bit):
                    n = (k // (2 * bit)) * bit + k % bit
                    for q in range(1, stages + 1):
                        if q < stages:
                            mark = orders(u, G)[q]
                            before = [b for b in orders(u, G)[1:q]]
                        else:
                            mark, before = 0, orders(u, G)[1:]
                        hit = True
                        for b in before:
                            hit = both_true(hit, (k // b) % 2 == 0)
                        if mark:
                            hit = both_true(hit, (k // mark) % 2 == 1)

                        @pl.when(hit)
                        def _(q=q):
                            remote(part.at[slot, t, u, k], recv.at[j, t, u, n], r_tx.at[j],
                                   r_rx.at[j, t, q - 1], (flip(seq, bit), fsdp)).start()

            return carry

        lax.fori_loop(0, (high - low) * G, step, 0)

    def alive(u, q):
        bits = orders(u, G)[:q]
        return [k for k in range(G) if not any(k & b for b in bits)]

    def landing(u, q, k):
        return sum(len(alive(u, p + 1)) for p in range(q)) + alive(u, q + 1).index(k)

    def goes(u, k):
        for q, b in enumerate(orders(u, G)):
            if k & b:
                return q
        return stages

    def r_wait(j, t, q):
        units = sum(goes(0, k) for k in range(G) if goes(0, k) == q)
        spot = recv.at[j, t, :, pl.ds(0, units)]
        remote(spot, spot, r_tx.at[j], r_rx.at[j, t, q - 1], sibling).wait_recv()

    def total(j, t, u, upto, k, store):
        tile = 128

        def step(i, carry):
            r = rows(i, tile)
            value = part[j % SLOTS, t, u, k, r, :].astype(F32)
            for q in range(upto):
                value = value + recv[j, t, u, landing(u, q, k), r, :].astype(F32)
            store(r, value.astype(BF16))
            return carry

        lax.fori_loop(0, length // tile, step, 0)

    def stage(j, t):
        with jax.named_scope(f"stage_{j}_{t}"):
            stage_body(j, t)

    def stage_body(j, t):
        for q in range(1, stages):
            r_wait(j, t, q)
            for u in range(PAIR):
                bit = orders(u, G)[q]
                for k in reversed(alive(u, q)):
                    if k & bit:
                        def put(r, value, u=u, k=k):
                            part[j % SLOTS, t, u, k, r, :] = value

                        total(j, t, u, q, k, put)
                        n = landing(u, q, k ^ bit)
                        remote(part.at[j % SLOTS, t, u, k], recv.at[j, t, u, n], r_tx.at[j],
                               r_rx.at[j, t, goes(u, k ^ bit) - 1], (flip(seq, bit), fsdp)).start()

    def ret_copy(j):
        return remote(ret.at[j], fin.at[j], ret_tx.at[0], ret_rx.at[j], outward)

    def settle(j, t):
        with jax.named_scope(f"settle_{j}_{t}"):
            settle_body(j, t)

    def settle_body(j, t):
        r_wait(j, t, stages)
        for u in range(PAIR):
            def put(r, value, u=u):
                if t:
                    ret[j, r, pl.ds(u * HEAD, HEAD)] = value
                else:
                    fin[j, r, pl.ds(u * HEAD, HEAD)] = value

            total(j, t, u, stages, 0, put)
        if t:
            ret_copy(j).start()

    def returned(j):
        if fold:
            @pl.when(guest)
            def _():
                with jax.named_scope(f"returned_{j}"):
                    remote(fin.at[j], fin.at[j], ret_tx.at[0], ret_rx.at[j], sibling).wait_recv()

    def sent(j):
        p = part.at[j % SLOTS, :, :, pl.ds(0, G - 1)]
        remote(p, p, r_tx.at[j], r_rx.at[j, 0, 0], sibling).wait_send()

    relayed = G == 4
    near = [1, 2] if relayed else list(range(1, G))

    def h_spot(owner, j):
        return heads.at[:, rows(owner * (C - 1) + j - 1, cw)]

    def h_half(owner, j, u):
        return heads.at[:, rows((owner * (C - 1) + j - 1) * PAIR + u, HEAD)]

    def h_copy(j, k):
        spot = h_spot(seq, j)
        return remote(spot, spot, h_tx.at[0], h_rx.at[j, 0], (flip(seq, k), fsdp))

    def h_relay(j, u):
        came, then = orders(u, G)[:2]
        half = h_half(flip(seq, came), j, u)
        return remote(half, half, h_tx.at[0], h_rx.at[j, 1], (flip(seq, then), fsdp))

    def h_wait(j):
        with jax.named_scope(f"hwait_{j}"):
            spot = heads.at[:, pl.ds(0, len(near) * cw)]
            remote(spot, spot, h_tx.at[0], h_rx.at[j, 0], sibling).wait_recv()

    def relay(j):
        h_wait(j)
        if relayed:
            for u in range(PAIR):
                send(True, lambda u=u: h_relay(j, u))

    def h_last(j):
        if relayed:
            with jax.named_scope(f"hlast_{j}"):
                spot = h_spot(seq, j)
                remote(spot, spot, h_tx.at[0], h_rx.at[j, 1], sibling).wait_recv()

    def attend(j, condition=True):
        when(condition, lambda: mix(j))

    def mix(j):
        with jax.named_scope(f"attend_{j}"):
            mix_body(j)

    def mix_body(j):
        tile = 256

        def one_head(h, carry):
            column = rows(h, HEAD)
            for i in range(length // tile):
                seen = (i + 1) * tile
                q = fin[j, pl.ds(i * tile, tile), column]
                scores = lax.dot_general(
                    q, fin[0, pl.ds(0, seen), pl.ds(0, HEAD)],
                    (((1,), (1,)), ((), ())), preferred_element_type=F32) * (HEAD ** -0.5)
                row = lax.broadcasted_iota(jnp.int32, (tile, seen), 0) + i * tile
                col = lax.broadcasted_iota(jnp.int32, (tile, seen), 1)
                scores = jnp.where(row >= col, scores, F32(-1e30))
                top = jnp.max(scores, axis=-1, keepdims=True)
                weights = jnp.exp(scores - top)
                probs = weights * (1.0 / jnp.sum(weights, axis=-1, keepdims=True))
                mixed = jnp.dot(probs.astype(BF16), fin[0, pl.ds(0, seen), pl.ds(HEAD, HEAD)],
                                preferred_element_type=F32)
                spot = rows((seq * (C - 1) + j - 1) * PAIR + h, HEAD)
                heads[pl.ds(i * tile, tile), spot] = mixed.astype(BF16)
            return carry

        lax.fori_loop(0, PAIR, one_head, 0)
        for k in near:
            h_copy(j, k).start()

    def target(c, h):
        b = seq * plan.devices + c
        if not plan.flat:
            return out.at[b]
        return out.at[:, rows(b * plan.parts + h, pw)]

    def n_load(o, own, h, r, spot, sems):
        copies = []
        for n in range(CORES):
            c = core if n == 0 else 1 - core
            cut = pl.ds(h * pw, pw)
            source = wo.at[r, cut] if own and n == 0 else gathered.at[o * CORES + c, r, cut]
            where = spot.at[0, :, pl.ds(n * pw, pw)] if plan.flat else spot.at[n]
            copies.append(pltpu.make_async_copy(source, where, sems.at[h, n]))
        return copies

    def br_spot(o, h, n, r):
        if plan.flat:
            return br.at[o, h, 0, r, pl.ds(n * pw, pw)]
        return br.at[o, h, n, r, :]

    def br_send(o, h, ordered=False):
        for n in range(CORES):
            c = n if ordered else (core if n == 0 else 1 - core)
            for k in range(1, G):
                d = flip(seq, k)
                remote(br_spot(o, h, n, rows(d, count)), target(o * CORES + c, h),
                       b_tx.at[0], b_rx.at[0], (d, fsdp)).start()
            pltpu.make_async_copy(br_spot(o, h, n, rows(seq, count)), target(o * CORES + c, h),
                                  b_loc.at[0]).start()

    tile = 256
    ahead, late = (C - 2) * cw, cw

    def strips(i, o, own, start, size, place, sems):
        for h in range(plan.parts):
            for d in range(G):
                r = pl.ds(d * (C - 1) * cw + start, size)
                for copy in n_load(o, own, h, r, place(h, d), sems):
                    copy.start()

    def strips_wait(place, sems):
        for h in range(plan.parts):
            for n in range(CORES):
                spot = place(h)
                where = spot.at[0, :, pl.ds(n * pw, pw)] if plan.flat else spot.at[n]
                pltpu.make_async_copy(where, where, sems.at[h, n]).wait()

    def early_load(i):
        o = stop if i == 0 else origin(i)
        strips(i, o, i == 0, ahead, late,
               lambda h, d: nv_late.at[i % plan.kept, h, :, pl.ds(d * late, late), :], nl_sem)
        if ahead:
            strips(i, o, i == 0, 0, ahead,
                   lambda h, d: nv.at[h, :, pl.ds(d * ahead, ahead), :], nv_sem)

    def branch_early(i):
        with jax.named_scope(f"early_{i}"):
            strips_wait(lambda h: nv_late.at[i % plan.kept, h], nl_sem)
            if ahead:
                strips_wait(lambda h: nv.at[h, :, pl.ds(0, G * ahead), :], nv_sem)
                for h in range(plan.parts):
                    for unit in range(plan.units):
                        def step(t, carry, h=h, unit=unit):
                            r = rows(t, tile)
                            acc = None
                            for d in range(G):
                                p = jnp.dot(heads[r, pl.ds(d * (C - 1) * cw, ahead)],
                                            nv[h, unit, pl.ds(d * ahead, ahead), :],
                                            preferred_element_type=F32)
                                acc = p if acc is None else acc + p
                            br_acc[i % plan.kept, h, unit, r, :] = acc
                            return carry

                        lax.fori_loop(0, length // tile, step, 0)

    def branch(i):
        with jax.named_scope(f"branch_{i}"):
            o = stop if i == 0 else origin(i)
            for h in range(plan.parts):
                for unit in range(plan.units):
                    def step(t, carry, h=h, unit=unit):
                        r = rows(t, tile)
                        acc = br_acc[i % plan.kept, h, unit, r, :] if ahead else None
                        for d in range(G):
                            p = jnp.dot(heads[r, pl.ds(d * (C - 1) * cw + ahead, late)],
                                        nv_late[i % plan.kept, h, unit, pl.ds(d * late, late), :],
                                        preferred_element_type=F32)
                            acc = p if acc is None else acc + p
                        br[o, h, unit, r, :] = acc.astype(BF16)
                        return carry

                    lax.fori_loop(0, length // tile, step, 0)
                br_send(o, h)

    def branch_last(i):
        o = origin(i)

        def loads(pc):
            cut = pl.ds(pc % per_part * piece, piece)
            h = pc // per_part
            return n_load(o, False, h, cut, nv.at[h, :, cut, :], nl_sem if pc % 2 else nv_sem)

        begun = 0

        def begin(last):
            nonlocal begun
            while begun <= min(last, PIECES - 1):
                polls(i, begun, begun + 1)
                with jax.named_scope(f"nsib_{i}_{begun}"):
                    n_across_wait(i, begun)
                if not fold:
                    for copy in loads(begun):
                        copy.start()
                begun += 1

        for pc in range(PIECES):
            begin(pc + 1 if pc < PIECES - 2 else pc)
            h, q = pc // per_part, pc % per_part
            if not fold:
                for copy in loads(pc):
                    copy.wait()
            for unit in range(plan.units):
                def step(i, carry, h=h, q=q, unit=unit):
                    r = rows(i, tile)
                    cut = pl.ds(q * piece, piece)
                    w = nl[h, cut, :] if fold else nv[h, unit, cut, :]
                    acc = jnp.dot(heads[r, cut], w, preferred_element_type=F32)
                    if q:
                        acc = acc + br_acc[plan.kept, h, unit, r, :]
                    if q < per_part - 1:
                        br_acc[plan.kept, h, unit, r, :] = acc
                    else:
                        br[o, h, unit, r, :] = acc.astype(BF16)
                    return carry

                lax.fori_loop(0, length // tile, step, 0)
            if q == per_part - 1:
                br_send(o, h, fold)

    def both(action):
        for t in reversed(range(turns)):
            action(t)

    early = min(2, C)

    def both_early(action):
        for j in range(early):
            action(j, 1)

    def take_chunk(j):
        for i in range(2, S):
            w_arrive(i, j)
        w_other_core(j)

    for j in range(early):
        w_arrive(1, j)
    for pc in range(FILL):
        n_own_in(host, pc)
    if early < C:
        w_own_in(host, early)
    for j in range(early):
        take_chunk(j)
        if j == 0:
            when(host, lambda: [x_wait(k) for k in range(G)])
        when(host, lambda j=j: project(j, 0, 1))
        if j == 0:
            for pc in range(PIECES):
                send(True, lambda pc=pc: n_across(0, pc))

    def own_early():
        for j in range(early):
            stage(j, 0)
        for j in range(early):
            settle(j, 0)
        for j in range(1, early):
            mix(j)

    def guests_early():
        with jax.named_scope("gwait"):
            r = nrm.at[1]
            remote(r, r, g_tx.at[0], g_rx.at[0], sibling).wait_recv()
        for j in range(early):
            project(j, 1, 2)

    when(host, own_early)
    taken = []
    relays = [j for j in range(1, C)]

    def polls(i, first, last, role=None):
        for pc in range(first * PIECES // 8, min(last, 8) * PIECES // 8):
            for who, name in ((host, "host"), (guest, "guest")):
                if (i, pc, name) in taken or i >= S or role not in (None, name):
                    continue
                if name == "host" and role is None and (i, pc, "guest") not in taken:
                    taken.extend([(i, pc, "host"), (i, pc, "guest")])
                    n_arrive(i, pc)
                elif name == "host" or fold:
                    taken.append((i, pc, name))
                    n_arrive(i, pc, who)

    def gather(i):
        if i:
            polls(i, 0, 8)
        with jax.named_scope(f"nsib_{i}"):
            n_across_wait(i)

    def relay_to(j):
        while relays and relays[0] <= j:
            relay(relays.pop(0))

    def close(j):
        when(host, lambda: both(lambda t: settle(j, t)))
        returned(j)

    sent_in = FILL

    def fill(count):
        nonlocal sent_in
        for pc in range(sent_in, min(PIECES, sent_in + count)):
            n_own_in(host, pc)
        sent_in = min(PIECES, sent_in + count)

    def forward(j):
        if early <= j < C:
            w_arrive(1, j)
            if j + 1 < C:
                fill((PIECES - TAIL - sent_in) // (C - 1 - j))
                w_own_in(host, j + 1)

    def attend_to(j):
        close(j)
        attend(j)

    polls(2, 0, 2, "host")
    if fold:
        when(host, guests_early)
    polls(2, 2, 4, "host")
    forward(early)
    if fold:
        when(host, lambda: both_early(stage))
        when(host, lambda: both_early(settle))
    forward(early + 1)
    if fold:
        polls(1, 0, 8, "guest")
        polls(2, 0, 4, "guest")
        for e in range(early):
            returned(e)
        for e in range(1, early):
            attend(e, guest)
    for j in range(early, C):
        take_chunk(j)
        last = j == C - 1
        if last:
            polls(1, 6, 8, "host")
            relay_to(j - 1)
            if fold:
                polls(2, 0, 8 - TAIL, "guest")
                gather(0)
                early_load(0)
        if j >= SLOTS:
            when(host, lambda j=j: sent(j - SLOTS))
        if last and fold:
            when(host, lambda j=j: project(j, 1, 2))
            polls(2, 8 - TAIL, 8, "host")
        else:
            when(host, lambda j=j: project(j, 0, turns))
        if last:
            break
        relay_to(j - 2)
        when(host, lambda j=j: both(lambda t: stage(j, t)))
        if j == early:
            for e in range(early + 2, C):
                forward(e)
            fill(PIECES)
            polls(2, 4, 6, "host")
        if j == C - 2:
            polls(2, 6, 8 - TAIL, "host")
            polls(1, 0, 6, "host")
        attend_to(j)
        if j == early:
            polls(2, 4, 6, "guest")
    fill(PIECES)
    relay_to(C - 2)
    two_steps = fold and C > early
    polls(3, 0, 1, "host")
    for j in range(1, C - 1):
        h_last(j)
    if two_steps:
        branch_early(0)
        gather(1)
        early_load(1)
        when(host, lambda: stage(C - 1, 1))
        when(host, lambda: project(C - 1, 0, 1))
        polls(3, 1, 2, "host")
        branch_early(1)
        gather(2)
        early_load(2)
        when(host, lambda: settle(C - 1, 1))
        returned(C - 1)
        attend(C - 1, guest)
        polls(3, 2, 3, "host")
        branch_early(2)
        when(host, lambda: stage(C - 1, 0))
        polls(3, 3, 4, "host")
        when(host, lambda: settle(C - 1, 0))
        attend(C - 1, host)
        polls(3, 4, 5, "host")
        polls(3, 0, 3, "guest")
    elif C > early:
        when(host, lambda: both(lambda t: stage(C - 1, t)))
        attend_to(C - 1)
    relay_to(C - 1)
    polls(3, 5, 6, "host")
    h_last(C - 1)
    polls(3, 6, 7, "host")
    for i in range(S - 1):
        if not two_steps:
            gather(i)
            early_load(i)
            branch_early(i)
        branch(i)
    polls(3, 0, 8, "host")
    polls(3, 3, 6, "guest")
    if S > 1:
        branch_last(S - 1)

    def all_of(side):
        span = plan.devices * plan.cols_out
        return out.at[:, rows(side, span)] if plan.flat else out.at[rows(side, plan.devices)]

    def left(sem, count, spot):
        def wait():
            t = spot(count)
            remote(t, t, sem.at[0], r_rx.at[0, 0, 0], sibling).wait_send()

        return wait

    with jax.named_scope("sends"):
        def w_spot(n):
            return gw.at[:, pl.ds(0, n * depth), :]

        def n_spot(n):
            return gathered.at[pl.ds(0, n)]

        for v in range(S // 2):
            there = far == v
            pl.when(there)(left(n_in, 1 + v, n_spot))
            pl.when(there)(left(w_in, 1 + v, w_spot))
            if v:
                pl.when(there)(left(n_out, S - v, n_spot))
                if not fold:
                    pl.when(there)(left(w_out, S - v, w_spot))
        left(n_sib, S, n_spot)()
        when(host, left(w_sib, S, w_spot))
        left(x_tx, G - 1, lambda n: tok.at[:, pl.ds(0, n * width)])()
        left(h_tx, G - 1, lambda n: heads.at[:, pl.ds(0, n * lw)])()
        if fold:
            pl.when(guest)(left(g_tx, 0, lambda n: nrm.at[0]))
            pl.when(host)(left(ret_tx, 0, lambda n: ret))
        when(host, lambda: [sent(j) for j in range(max(0, C - SLOTS), C)])

    def others(first, n):
        if plan.flat:
            return out.at[:, pl.ds(first, n * plan.devices * plan.cols_out)]
        return out.at[pl.ds(first, n * plan.devices)]

    with jax.named_scope("bwait"):
        spot = others(0, G - 1)
        remote(spot, spot, b_tx.at[0], b_rx.at[0], sibling).wait()
        spot = others(0, 1)
        pltpu.make_async_copy(spot, spot, b_loc.at[0]).wait()


def body(tokens, norm_gain, w_query, key_weight, value_weight, w_out):
    group, devices = lax.axis_size("seq"), lax.axis_size("fsdp")
    plan = Plan(group, devices, tokens[0], w_query, key_weight, w_out)
    G, S, C, T = plan.group, plan.stops, plan.chunks, plan.turns
    length, cw = plan.length, plan.chunk
    unit_cols = plan.part_cols * CORES // plan.units
    any_space = pl.BlockSpec(memory_space=pl.ANY)
    dma = pltpu.SemaphoreType.DMA
    if plan.flat:
        out_shape = (plan.count, plan.features)
    else:
        out_shape = (G * devices, plan.count, plan.cols_out)
    stages = len(orders(0, G))
    nv_rows = max(16, G * (C - 2) * cw) if plan.fold else plan.rows_out
    branches, _ = pl.pallas_call(
        functools.partial(kernel, plan),
        out_shape=(
            jax.ShapeDtypeStruct(out_shape, BF16),
            jax.ShapeDtypeStruct((devices,) + w_out.shape, BF16),
        ),
        in_specs=[any_space, pl.BlockSpec(memory_space=pltpu.VMEM)] + [any_space] * 4,
        out_specs=(any_space, any_space),
        scratch_shapes=[
            pltpu.VMEM((plan.count, plan.features), BF16),
            pltpu.VMEM((C, plan.width, G * cw), BF16),
            pltpu.VMEM((T, length, plan.width), BF16),
            pltpu.VMEM((SLOTS, T, PAIR, G, length, HEAD), BF16),
            pltpu.VMEM((C, T, PAIR, G - 1, length, HEAD), BF16),
            pltpu.VMEM((C, length, cw), BF16),
            pltpu.VMEM((C if plan.fold else 1, length, cw), BF16),
            pltpu.VMEM((length, plan.rows_out), BF16),
            pltpu.VMEM((plan.parts, plan.units, nv_rows, unit_cols), BF16),
            pltpu.VMEM((plan.kept, plan.parts, plan.units, G * cw, unit_cols), BF16),
            pltpu.VMEM((plan.parts, plan.rows_out if plan.fold else 16, unit_cols), BF16),
            pltpu.VMEM((S, plan.parts, plan.units, length, unit_cols), BF16),
            pltpu.VMEM((plan.kept + 1, plan.parts, plan.units, length, unit_cols), F32),
            dma((C, S + 1)), dma((1,)), dma((1,)), dma((1,)), dma((C,)),
            dma((S + 2, max(PIECES, S))), dma((1,)), dma((1,)), dma((1,)),
            dma((G,)), dma((1,)), dma((2,)), dma((1,)), dma((1,)),
            dma((C, T, stages)), dma((C,)), dma((C,)), dma((1,)),
            dma((C, 2)), dma((1,)), dma((1,)), dma((1,)), dma((1,)), dma((plan.parts, CORES)), dma((plan.parts, CORES)),
        ],
        compiler_params=pltpu.CompilerParams(
            collective_id=0, has_side_effects=True, vmem_limit_bytes=67043328),
    )(tokens[0], norm_gain[None], w_query, key_weight, value_weight, w_out)
    if not plan.flat:
        branches = jnp.transpose(branches, (1, 0, 2)).reshape(plan.count, plan.features)
    return tokens.astype(F32) + branches[None].astype(F32)


def solution(mesh):
    placed = (
        P("fsdp", "seq", None),
        P(),
        P(("seq", "fsdp"), None),
        P(("seq", "fsdp"), None),
        P(("seq", "fsdp"), None),
        P(None, ("seq", "fsdp")),
    )
    return jax.shard_map(
        body, mesh=mesh, in_specs=placed, out_specs=P("fsdp", "seq", None), check_vma=False
    )
```
